128 devices in a mesh: col: 2 (over core), row: 64 (over z, y, x).
Axes of the slice: x: 4, y: 4, z: 4, core: 2. Of those that a mesh axis runs over, the one named last changes fastest.
Arguments:
- forcing: float32 [2, 1536, 48, 256], P(None, 'row', 'col')
- init_guess: float32 [2, 1536, 48, 256], P(None, 'row', 'col')
- cell_coef: float32 [2, 1536, 48], P(None, 'row', 'col')
- solve_rows: bfloat16 [2, 64, 2, 576, 784], P(None, 'row', 'col')
- relax_factor: float32 [2], replicated
Outputs:
- output: float32 [2, 1536, 48, 256], P(None, 'row', 'col')
All inputs are finite; a program needn't handle non-finite values.
Results may differ from the reference program's by a relative error of at most 0.001.
Values are sent between devices in bfloat16 or wider.
A program may use at most 1 GiB of HBM per device.

```python
import jax
import jax.numpy as jnp
from jax import lax

SUBDOMAIN = 24
MARGIN = 2
RHS_PER_SYS = 256
SWEEPS = 4
BLOCK_ROWS = 64
BLOCK_COLS = 2
SYSTEMS = 2

EXT_SIZE = SUBDOMAIN + 2 * MARGIN
GRID_ROWS = BLOCK_ROWS * SUBDOMAIN
GRID_COLS = BLOCK_COLS * SUBDOMAIN


def face_coefs(coef_grid):
    face_x = jnp.concatenate([coef_grid[:1], 0.5 * (coef_grid[:-1] + coef_grid[1:]), coef_grid[-1:]], axis=0)
    face_y = jnp.concatenate([coef_grid[:, :1], 0.5 * (coef_grid[:, :-1] + coef_grid[:, 1:]), coef_grid[:, -1:]], axis=1)
    return face_x, face_y


def apply_op(face_x, face_y, values):
    wide_x = jnp.pad(values, ((1, 1), (0, 0), (0, 0)))
    wide_y = jnp.pad(values, ((0, 0), (1, 1), (0, 0)))
    flux_x = face_x[:, :, None] * (wide_x[1:] - wide_x[:-1])
    flux_y = face_y[:, :, None] * (wide_y[:, 1:] - wide_y[:, :-1])
    return flux_x[:-1] - flux_x[1:] + flux_y[:, :-1] - flux_y[:, 1:]


def subdomain_inverses(coef_grid):
    face_x, face_y = face_coefs(coef_grid)
    diagonal = face_x[:-1] + face_x[1:] + face_y[:, :-1] + face_y[:, 1:]
    diag_pad = jnp.pad(diagonal, MARGIN, constant_values=1.0)
    couple_x = jnp.pad(face_x[1:-1], MARGIN)
    couple_y = jnp.pad(face_y[:, 1:-1], MARGIN)

    def one_block(block_id):
        row_start = (block_id // BLOCK_COLS) * SUBDOMAIN
        col_start = (block_id % BLOCK_COLS) * SUBDOMAIN
        diag_blk = lax.dynamic_slice(diag_pad, (row_start, col_start), (EXT_SIZE, EXT_SIZE)).reshape(-1)
        link_x = lax.dynamic_slice(couple_x, (row_start, col_start), (EXT_SIZE - 1, EXT_SIZE)).reshape(-1)
        link_y = lax.dynamic_slice(couple_y, (row_start, col_start), (EXT_SIZE, EXT_SIZE - 1))
        link_y = jnp.pad(link_y, ((0, 0), (0, 1))).reshape(-1)[:-1]
        local_op = jnp.diag(diag_blk) - jnp.diag(link_x, EXT_SIZE) - jnp.diag(link_x, -EXT_SIZE) - jnp.diag(link_y, 1) - jnp.diag(link_y, -1)
        full_inv = jnp.linalg.inv(local_op)
        own_rows = full_inv.reshape(EXT_SIZE, EXT_SIZE, EXT_SIZE * EXT_SIZE)[MARGIN:MARGIN + SUBDOMAIN, MARGIN:MARGIN + SUBDOMAIN]
        return own_rows.reshape(SUBDOMAIN * SUBDOMAIN, EXT_SIZE * EXT_SIZE)

    blocks = lax.map(one_block, jnp.arange(BLOCK_ROWS * BLOCK_COLS))
    return blocks.reshape(BLOCK_ROWS, BLOCK_COLS, SUBDOMAIN * SUBDOMAIN, EXT_SIZE * EXT_SIZE)


def setup_inputs(seed: int = 0) -> dict:
    base_key = jax.random.key(seed)
    key_f, key_u, key_c, key_w = jax.random.split(base_key, 4)
    grid_shape = (SYSTEMS, GRID_ROWS, GRID_COLS, RHS_PER_SYS)
    forcing = jax.random.normal(key_f, grid_shape, jnp.float32)
    init_guess = 0.5 * jax.random.normal(key_u, grid_shape, jnp.float32)
    cell_coef = jnp.exp(1.2 * jax.random.uniform(key_c, (SYSTEMS, GRID_ROWS, GRID_COLS), jnp.float32, -1.0, 1.0))
    relax_factor = jax.random.uniform(key_w, (SYSTEMS,), jnp.float32, 0.35, 0.6)
    solve_rows = jnp.stack([subdomain_inverses(cell_coef[system]) for system in range(SYSTEMS)]).astype(jnp.bfloat16)
    return {"forcing": forcing, "init_guess": init_guess, "cell_coef": cell_coef, "solve_rows": solve_rows, "relax_factor": relax_factor}


def solve_system(rhs_grid, start_guess, coef_grid, inv_rows, step_size):
    face_x, face_y = face_coefs(coef_grid)
    flat_rows = inv_rows.reshape(BLOCK_ROWS * BLOCK_COLS, SUBDOMAIN * SUBDOMAIN, EXT_SIZE * EXT_SIZE)
    block_ids = jnp.arange(BLOCK_ROWS * BLOCK_COLS)

    def one_sweep(sweep_state, unused):
        approx, residual = sweep_state
        padded = jnp.pad(residual.astype(jnp.bfloat16), ((MARGIN, MARGIN), (MARGIN, MARGIN), (0, 0)))

        def block_solve(operands):
            block_id, block_mat = operands
            row_start = (block_id // BLOCK_COLS) * SUBDOMAIN
            col_start = (block_id % BLOCK_COLS) * SUBDOMAIN
            window = lax.dynamic_slice(padded, (row_start, col_start, 0), (EXT_SIZE, EXT_SIZE, RHS_PER_SYS))
            return jnp.dot(block_mat, window.reshape(EXT_SIZE * EXT_SIZE, RHS_PER_SYS), preferred_element_type=jnp.float32)

        correction = lax.map(block_solve, (block_ids, flat_rows))
        correction = correction.reshape(BLOCK_ROWS, BLOCK_COLS, SUBDOMAIN, SUBDOMAIN, RHS_PER_SYS).transpose(0, 2, 1, 3, 4).reshape(GRID_ROWS, GRID_COLS, RHS_PER_SYS)
        approx = approx + step_size * correction
        residual = residual - step_size * apply_op(face_x, face_y, correction)
        return (approx, residual), None

    residual = rhs_grid - apply_op(face_x, face_y, start_guess)
    (approx, _), _ = lax.scan(one_sweep, (start_guess, residual), None, length=SWEEPS)
    return approx


def reference(forcing, init_guess, cell_coef, solve_rows, relax_factor):
    results = [solve_system(forcing[system], init_guess[system], cell_coef[system], solve_rows[system], relax_factor[system]) for system in range(SYSTEMS)]
    return jnp.stack(results)
```

```python
import functools

import jax
import jax.numpy as jnp
from jax import lax
from jax.experimental import pallas as pl
from jax.experimental.pallas import tpu as pltpu
from jax.sharding import PartitionSpec as P

SWEEPS = 4
SUB = 24
MARGIN = 2
EXT = SUB + 2 * MARGIN
BAND = 2 * SUB
EDGE = 3
WIN = EXT * BAND
WIN_PAD = 1408
LANES = 128
F32 = jnp.float32
BF16 = jnp.bfloat16
MESH = pl.DeviceIdType.MESH

EDGE_ROWS = tuple(range(EDGE)) + tuple(range(SUB - EDGE, SUB))
INNER_ROWS = tuple(range(EDGE, SUB - EDGE))


def kernel(rows, halves, f_hbm, u_hbm, c_hbm, s_hbm, om_ref, out_hbm, res, cor, app, s_raw, s_edge, s_inner, win, c_raw, c_nbr, c_wide,
           face_x, face_lo, face_hi, diag, send_f, send_b, recv_f, recv_b, loc_sem, side_send, side_recv, csend, crecv, fsend, frecv,
           bsend, brecv):
    core = lax.axis_index("col")
    row = lax.axis_index("row")
    other = 1 - core
    width = 2 * LANES // halves
    has = (row > 0, row < rows - 1)
    near = (row - 1, row + 1)

    mine = pl.multiple_of(core * SUB, 8)
    loads = [
        pltpu.make_async_copy(c_hbm.at[core], c_raw.at[core], loc_sem.at[0]),
        pltpu.make_async_copy(f_hbm.at[core], res.at[:, pl.ds(mine, SUB), :], loc_sem.at[1]),
        pltpu.make_async_copy(u_hbm.at[core], cor.at[:, pl.ds(mine, SUB), :], loc_sem.at[2]),
        pltpu.make_async_copy(s_hbm.at[core], s_raw.at[core], loc_sem.at[3]),
    ]
    for load in loads:
        load.start()

    barrier = pltpu.get_barrier_semaphore()
    pl.semaphore_signal(barrier, inc=1, device_id={"col": other}, device_id_type=MESH)
    for way in range(2):
        @pl.when(has[way])
        def _():
            pl.semaphore_signal(barrier, inc=1, device_id={"row": near[way]}, device_id_type=MESH)
    pl.semaphore_wait(barrier, 1 + has[0].astype(jnp.int32) + has[1].astype(jnp.int32))

    def swap(src, dst, index):
        return pltpu.make_async_remote_copy(src, dst, side_send.at[index], side_recv.at[index], device_id={"col": other}, device_id_type=MESH)

    swaps = [
        swap(c_hbm.at[other], c_raw.at[core], 0),
        swap(f_hbm.at[other], res.at[:, pl.ds(mine, SUB), :], 1),
        swap(u_hbm.at[other], cor.at[:, pl.ds(mine, SUB), :], 2),
        swap(s_hbm.at[other], s_raw.at[core], 3),
    ]
    for item in swaps:
        item.start()

    win[WIN:, :] = jnp.zeros((WIN_PAD - WIN, 2 * LANES), BF16)
    for way in range(2):
        @pl.when(jnp.logical_not(has[way]))
        def _():
            for rnd in range(SWEEPS):
                recv_f[rnd, way] = jnp.zeros(recv_f.shape[2:], F32)
                recv_b[rnd, way] = jnp.zeros(recv_b.shape[2:], BF16)

    loads[0].wait()
    swaps[0].wait()
    for way in range(2):
        @pl.when(has[way])
        def _():
            pltpu.make_async_remote_copy(c_raw, c_nbr.at[1 - way], csend.at[way], crecv.at[1 - way], device_id={"row": near[way]}, device_id_type=MESH).start()

    eye = lax.broadcasted_iota(jnp.int32, (SUB, SUB), 0) == lax.broadcasted_iota(jnp.int32, (SUB, SUB), 1)

    def column(ref, block, x):
        line = jnp.broadcast_to(ref[block, pl.ds(x, 1), :], (SUB, SUB))
        return jnp.broadcast_to(jnp.sum(jnp.where(eye, line, 0.0), axis=1, keepdims=True), (SUB, LANES))

    for x in range(SUB):
        for block in range(2):
            c_wide[x, SUB * block:SUB * (block + 1), :] = column(c_raw, block, x)
    cell = lax.broadcasted_iota(jnp.int32, (BAND, LANES), 0)
    for x in range(SUB):
        own = c_wide[x]
        below = pltpu.roll(own, 1, 0)
        above = pltpu.roll(own, BAND - 1, 0)
        lo = 0.5 * (own + below)
        hi = 0.5 * (own + above)
        total = jnp.where(cell == 0, own, lo) + jnp.where(cell == BAND - 1, own, hi)
        face_lo[x] = jnp.where(cell == 0, 0.0, lo)
        face_hi[x] = jnp.where(cell == BAND - 1, 0.0, hi)
        if x > 0:
            low_x = 0.5 * (c_wide[x - 1] + own)
            face_x[x] = low_x
            total = total + low_x
        if x < SUB - 1:
            total = total + 0.5 * (own + c_wide[x + 1])
        diag[x] = total

    def lanes_of(half):
        return [slice(half * width + LANES * i, half * width + LANES * (i + 1)) for i in range(width // LANES)]

    def neighbourless(x, lanes, last_static=None):
        here = cor[x, :, lanes]
        flux = diag[x] * here - face_lo[x] * pltpu.roll(here, 1, 0) - face_hi[x] * pltpu.roll(here, BAND - 1, 0)
        if last_static is None or x > 0:
            flux = flux - face_x[x] * cor[x - 1, :, lanes]
        if last_static is None or x < SUB - 1:
            flux = flux - face_x[x + 1] * cor[x + 1, :, lanes]
        return flux

    edge_row = (0, SUB - 1)
    second_row = (1, SUB - 2)

    def message(rnd, way, half):
        lane = pl.ds(half * width, width)
        return (
            pltpu.make_async_remote_copy(send_f.at[rnd, way, :, :, lane], recv_f.at[rnd, 1 - way, :, :, lane], fsend.at[rnd, way, half],
                                         frecv.at[rnd, 1 - way, half], device_id={"row": near[way]}, device_id_type=MESH),
            pltpu.make_async_remote_copy(send_b.at[rnd, way, :, lane], recv_b.at[rnd, 1 - way, :, lane], bsend.at[rnd, way, half],
                                         brecv.at[rnd, 1 - way, half], device_id={"row": near[way]}, device_id_type=MESH),
        )

    def send_edges(rnd, half, omega):
        for way in range(2):
            x, y = edge_row[way], second_row[way]
            for lanes in lanes_of(half):
                first = res[x, :, lanes] - omega * neighbourless(x, lanes, True)
                second = res[y, :, lanes] - omega * neighbourless(y, lanes, True)
                res[x, :, lanes] = first
                res[y, :, lanes] = second
                send_f[rnd, way, 0, :, lanes] = cor[x, :, lanes]
                send_f[rnd, way, 1, :, lanes] = first
                send_b[rnd, way, :, lanes] = second.astype(BF16)

            @pl.when(has[way])
            def _():
                for copy in message(rnd, way, half):
                    copy.start()

    def inner_update(rnd, half, omega):
        def body(x, carry):
            for lanes in lanes_of(half):
                new = res[x, :, lanes] - omega * neighbourless(x, lanes)
                res[x, :, lanes] = new
                win[pl.ds(pl.multiple_of((x + MARGIN) * BAND, 16), BAND), lanes] = new.astype(BF16)
            return carry
        lax.fori_loop(2, SUB - 2, body, 0)
        for x in second_row:
            for lanes in lanes_of(half):
                win[(x + MARGIN) * BAND:(x + MARGIN + 1) * BAND, lanes] = res[x, :, lanes].astype(BF16)

    def take_edges(rnd, half, omega):
        for way in range(2):
            @pl.when(has[way])
            def _():
                for copy in message(rnd, 1 - way, half):
                    copy.wait_recv()
        for way in range(2):
            x = edge_row[way]
            face = face_x[0] if way == 0 else face_x[SUB]
            outer, beyond = (1, 0) if way == 0 else (EXT - 2, EXT - 1)
            for lanes in lanes_of(half):
                flux = omega * face * (cor[x, :, lanes] - recv_f[rnd, way, 0, :, lanes])
                new = res[x, :, lanes] - flux
                res[x, :, lanes] = new
                win[(x + MARGIN) * BAND:(x + MARGIN + 1) * BAND, lanes] = new.astype(BF16)
                win[outer * BAND:(outer + 1) * BAND, lanes] = (recv_f[rnd, way, 1, :, lanes] + flux).astype(BF16)
                win[beyond * BAND:(beyond + 1) * BAND, lanes] = recv_b[rnd, way, :, lanes]

    def solve(mat, which, half):
        count = len(which) * SUB
        for block in range(2):
            part = jnp.dot(mat[block], win[:, half * width:(half + 1) * width], preferred_element_type=F32)
            for i, x in enumerate(which):
                cor[x, SUB * block:SUB * (block + 1), half * width:(half + 1) * width] = part[SUB * i:SUB * (i + 1)]

    for item in loads[1:3]:
        item.wait()
    for item in swaps[1:3]:
        item.wait()
    for half in range(halves):
        send_edges(0, half, 1.0)
    for half in range(halves):
        inner_update(0, half, 1.0)

    def keep(x, carry):
        app[x] = cor[x]
        return carry
    lax.fori_loop(0, SUB, keep, 0)

    loads[3].wait()
    swaps[3].wait()
    for chunk in range(0, WIN_PAD, 256):
        size = min(256, WIN_PAD - chunk)
        first = (chunk // BAND) * EXT // 16 * 16
        last = min(EXT * EXT, -(-min(EXT, (chunk + size - 1) // BAND + 1) * EXT // 16) * 16)
        source = lax.broadcasted_iota(jnp.int32, (last - first, size), 0) + first
        target = lax.broadcasted_iota(jnp.int32, (last - first, size), 1) + chunk
        ext_x = lax.shift_right_logical(source * 2341, 16)
        ext_y = source - EXT * ext_x
        for block in range(2):
            band_y = ext_y + (SUB * block - MARGIN)
            hit = (target == ext_x * BAND + band_y) & (band_y >= 0) & (band_y < BAND)
            pick = jnp.where(hit, 1.0, 0.0).astype(BF16)
            moved = lax.dot_general(s_raw[block, first:last, :], pick, (((0,), (0,)), ((), ())), preferred_element_type=F32)
            cut = EDGE * SUB
            s_edge[block, :, chunk:chunk + size] = jnp.concatenate([moved[:cut], moved[-cut:]], axis=0).astype(BF16)
            s_inner[block, :, chunk:chunk + size] = moved[cut:-cut].astype(BF16)

    for way in range(2):
        @pl.when(has[way])
        def _():
            pltpu.make_async_remote_copy(c_raw, c_nbr.at[way], csend.at[1 - way], crecv.at[way], device_id={"row": near[way]}, device_id_type=MESH).wait_recv()
        x = edge_row[way]
        at = 0 if way == 0 else SUB
        for block in range(2):
            part = slice(SUB * block, SUB * (block + 1))
            own = c_wide[x, part]
            beyond = jnp.where(has[way], column(c_nbr.at[way], block, edge_row[1 - way]), own)
            face_x[at, part] = 0.5 * (own + beyond)

    omega = om_ref[core]
    for sweep in range(SWEEPS):
        before = 1.0 if sweep == 0 else omega
        for half in range(halves):
            take_edges(sweep, half, before)
            solve(s_edge, EDGE_ROWS, half)
            if sweep < SWEEPS - 1:
                send_edges(sweep + 1, half, omega)
            solve(s_inner, INNER_ROWS, half)

            def advance(x, carry):
                for lanes in lanes_of(half):
                    app[x, :, lanes] = app[x, :, lanes] + omega * cor[x, :, lanes]
                return carry
            lax.fori_loop(0, SUB, advance, 0)
            if sweep < SWEEPS - 1:
                inner_update(sweep + 1, half, omega)

    theirs = pl.multiple_of(other * SUB, 8)
    back = pltpu.make_async_remote_copy(app.at[:, pl.ds(theirs, SUB), :], out_hbm.at[core], side_send.at[4], side_recv.at[4], device_id={"col": other}, device_id_type=MESH)
    back.start()
    keep_own = pltpu.make_async_copy(app.at[:, pl.ds(mine, SUB), :], out_hbm.at[core], loc_sem.at[4])
    keep_own.start()
    keep_own.wait()
    back.wait()
    for way in range(2):
        @pl.when(has[way])
        def _():
            pltpu.make_async_remote_copy(c_raw, c_nbr.at[1 - way], csend.at[way], crecv.at[1 - way], device_id={"row": near[way]}, device_id_type=MESH).wait_send()
            for rnd in range(SWEEPS):
                for half in range(halves):
                    for copy in message(rnd, way, half):
                        copy.wait_send()


def solution(mesh):
    rows = mesh.shape["row"]
    halves = 2
    grid_spec = P(None, "row", "col", None)

    def local_sweeps(forcing, init_guess, cell_coef, solve_rows, relax_factor):
        systems, _, _, rhs = forcing.shape
        solve_mat = jnp.swapaxes(solve_rows.reshape(systems, SUB * SUB, EXT * EXT), 1, 2)
        any_space = pl.BlockSpec(memory_space=pl.ANY)
        inner = SUB * len(INNER_ROWS)
        edge = SUB * len(EDGE_ROWS)
        return pl.pallas_call(
            functools.partial(kernel, rows, halves),
            out_shape=jax.ShapeDtypeStruct(forcing.shape, F32),
            in_specs=[any_space] * 4 + [pl.BlockSpec(memory_space=pltpu.SMEM)],
            out_specs=any_space,
            scratch_shapes=[
                pltpu.VMEM((SUB, BAND, rhs), F32),
                pltpu.VMEM((SUB, BAND, rhs), F32),
                pltpu.VMEM((SUB, BAND, rhs), F32),
                pltpu.VMEM((2, EXT * EXT, SUB * SUB), BF16),
                pltpu.VMEM((2, edge, WIN_PAD), BF16),
                pltpu.VMEM((2, inner, WIN_PAD), BF16),
                pltpu.VMEM((WIN_PAD, rhs), BF16),
                pltpu.VMEM((2, SUB, SUB), F32),
                pltpu.VMEM((2, 2, SUB, SUB), F32),
                pltpu.VMEM((SUB, BAND, LANES), F32),
                pltpu.VMEM((SUB + 1, BAND, LANES), F32),
                pltpu.VMEM((SUB, BAND, LANES), F32),
                pltpu.VMEM((SUB, BAND, LANES), F32),
                pltpu.VMEM((SUB, BAND, LANES), F32),
                pltpu.VMEM((SWEEPS, 2, 2, BAND, rhs), F32),
                pltpu.VMEM((SWEEPS, 2, BAND, rhs), BF16),
                pltpu.VMEM((SWEEPS, 2, 2, BAND, rhs), F32),
                pltpu.VMEM((SWEEPS, 2, BAND, rhs), BF16),
                pltpu.SemaphoreType.DMA((5,)),
                pltpu.SemaphoreType.DMA((5,)),
                pltpu.SemaphoreType.DMA((5,)),
                pltpu.SemaphoreType.DMA((2,)),
                pltpu.SemaphoreType.DMA((2,)),
                pltpu.SemaphoreType.DMA((SWEEPS, 2, halves)),
                pltpu.SemaphoreType.DMA((SWEEPS, 2, halves)),
                pltpu.SemaphoreType.DMA((SWEEPS, 2, halves)),
                pltpu.SemaphoreType.DMA((SWEEPS, 2, halves)),
            ],
            compiler_params=pltpu.CompilerParams(collective_id=0, has_side_effects=True, vmem_limit_bytes=60 * 1024 * 1024),
        )(forcing, init_guess, cell_coef, solve_mat, relax_factor)

    return jax.shard_map(local_sweeps, mesh=mesh, in_specs=(grid_spec, grid_spec, P(None, "row", "col"), P(None, "row", "col", None, None), P(None)), out_specs=grid_spec, check_vma=False)
```

```python
import functools

import jax
import jax.numpy as jnp
from jax import lax
from jax.experimental import pallas as pl
from jax.experimental.pallas import tpu as pltpu
from jax.sharding import PartitionSpec as P

SWEEPS = 4
SUB = 24
MARGIN = 2
EXT = SUB + 2 * MARGIN
BAND = 2 * SUB
SLOT = 32
OUTER = 8
INNER = EXT - OUTER
LANES = 128
RHS = 2 * LANES
HALVES = 2
F32 = jnp.float32
BF16 = jnp.bfloat16
MESH = pl.DeviceIdType.MESH

EDGE_ROWS = (0, 1, 2, SUB - 3, SUB - 2, SUB - 1)
ROW_ORDER = EDGE_ROWS + tuple(range(3, SUB - 3))
EDGE_CELLS = SUB * len(EDGE_ROWS)
CELLS = SUB * SUB
CHUNK = EDGE_CELLS
EDGE_ROW = (0, SUB - 1)
SECOND_ROW = (1, SUB - 2)
PLACES = ((0, 1, 2, 3), (7, 6, 5, 4))
FIRST = 80


def kernel(rows, f_hbm, u_hbm, c_hbm, s_hbm, om_ref, out_ref, res, cor, app, fin, pre, s_raw, s_out, s_in, w_out, w_in, c_own, c_raw, c_nbr,
           c_wide, c_part, face_x, face_lo, face_hi, cross, diag, u_edge, f_edge, send_0, recv_0, send_f, send_b, recv_f, recv_b,
           loc_sem, edge_sem, side_send, side_recv, csend, crecv, send0_sem, recv0_sem, fsend, frecv, bsend, brecv, back_send, back_recv):
    core = lax.axis_index("col")
    row = lax.axis_index("row")
    other = 1 - core
    sys = lax.rem(core + row, 2)
    systems = (sys, 1 - sys)
    has = (row > 0, row < rows - 1)
    near = (jnp.maximum(row - 1, 0), jnp.minimum(row + 1, rows - 1))
    mine = pl.multiple_of(core * SUB, 8)
    width = RHS // HALVES

    def lanes_of(half):
        return [slice(half * width + LANES * i, half * width + LANES * (i + 1)) for i in range(width // LANES)]

    all_lanes = [slice(LANES * i, LANES * (i + 1)) for i in range(RHS // LANES)]

    load_c = pltpu.make_async_copy(c_hbm, c_own, loc_sem.at[0])
    load_c.start()
    edge_loads = []
    for j in range(2):
        for way in range(2):
            edge_loads.append(pltpu.make_async_copy(u_hbm.at[systems[j], (SUB - 3) * way:(SUB - 3) * way + 3], u_edge.at[j, way], edge_sem.at[j, way, 0]))
            edge_loads.append(pltpu.make_async_copy(f_hbm.at[systems[j], (SUB - 2) * way:(SUB - 2) * way + 2], f_edge.at[j, way], edge_sem.at[j, way, 1]))
    for load in edge_loads:
        load.start()
    load_c_raw = pltpu.make_async_copy(c_hbm.at[sys], c_raw.at[core], loc_sem.at[4])
    load_s = pltpu.make_async_copy(s_hbm.at[sys], s_raw.at[core], loc_sem.at[3])
    load_f = pltpu.make_async_copy(f_hbm.at[sys], res.at[:, pl.ds(mine, SUB), :], loc_sem.at[1])
    load_u = pltpu.make_async_copy(u_hbm.at[sys], cor.at[:, pl.ds(mine, SUB), :], loc_sem.at[2])
    for load in (load_c_raw, load_s, load_f, load_u):
        load.start()

    barrier = pltpu.get_barrier_semaphore()
    for way in range(2):
        @pl.when(has[way])
        def _():
            for col in range(2):
                pl.semaphore_signal(barrier, inc=1, device_id=(col, near[way]), device_id_type=MESH)
    pl.semaphore_signal(barrier, inc=1, device_id={"col": other}, device_id_type=MESH)

    eye = lax.broadcasted_iota(jnp.int32, (SUB, SUB), 0) == lax.broadcasted_iota(jnp.int32, (SUB, SUB), 1)

    def column(ref, lead, x):
        line = jnp.broadcast_to(ref[lead + (pl.ds(x, 1), slice(None))], (SUB, SUB))
        return jnp.broadcast_to(jnp.sum(jnp.where(eye, line, 0.0), axis=1, keepdims=True), (SUB, LANES))

    load_c.wait()
    for j in range(2):
        for x in EDGE_ROWS:
            c_part[j, x] = column(c_own, (systems[j],), x)
    for load in edge_loads:
        load.wait()
    spot = lax.broadcasted_iota(jnp.int32, (SUB, LANES), 0)
    for j in range(2):
        for way in range(2):
            step = 1 if way == 0 else -1
            place = (0, 1, 2) if way == 0 else (2, 1, 0)
            into = (0, 1) if way == 0 else (1, 0)
            at = [EDGE_ROW[way] + step * i for i in range(3)]
            c = [c_part[j, x] for x in at]
            link = [0.5 * (c[0] + c[1]), 0.5 * (c[1] + c[2])]
            for i in range(2):
                lo = jnp.where(spot == 0, 0.0, 0.5 * (c[i] + pltpu.roll(c[i], 1, 0)))
                hi = jnp.where(spot == SUB - 1, 0.0, 0.5 * (c[i] + pltpu.roll(c[i], SUB - 1, 0)))
                wall = jnp.where((spot == 0) & (core == 0) | (spot == SUB - 1) & (core == 1), c[i], 0.0)
                total = lo + hi + wall + link[i]
                if i == 1:
                    total = total + link[0]
                for lanes in all_lanes:
                    u = [u_edge[j, way, place[n], :, lanes] for n in range(3)]
                    flux = total * u[i] - lo * pltpu.roll(u[i], 1, 0) - hi * pltpu.roll(u[i], SUB - 1, 0) - link[i] * u[i + 1]
                    if i == 1:
                        flux = flux - link[0] * u[0]
                    send_0[way, j, SUB * (i + 1):SUB * (i + 2), lanes] = f_edge[j, way, into[i], :, lanes] - flux
                    if i == 0:
                        send_0[way, j, 0:SUB, lanes] = u[0]
            tile = jnp.where(core == 0, u_edge[j, way, place[1], SUB - 8:SUB, :], u_edge[j, way, place[1], 0:8, :])
            send_0[way, j, 3 * SUB:FIRST, :] = tile

    source = lax.broadcasted_iota(jnp.int32, (4 * EXT, 4 * SLOT), 0)
    target = lax.broadcasted_iota(jnp.int32, (4 * EXT, 4 * SLOT), 1)
    ext_x = lax.shift_right_logical(source * 2341, 16)
    ext_y = source - EXT * ext_x

    def reorder(block):
        shift = (SUB - (BAND - SLOT)) * block - MARGIN
        inside = ext_y + SUB * block - MARGIN
        hit = (target == ext_x * SLOT + ext_y + shift) & (inside >= 0) & (inside < BAND)
        pick = jnp.where(hit, 1.0, 0.0).astype(BF16)
        groups = EXT // 4
        for group in range(groups):
            moved = lax.dot_general(s_raw[block, 4 * EXT * group:4 * EXT * (group + 1), :], pick, (((0,), (0,)), ((), ())), preferred_element_type=F32)
            cut = 3 * SUB
            moved = jnp.concatenate([moved[:cut], moved[-cut:], moved[cut:-cut]], axis=0).astype(BF16)
            if group == 0:
                s_out[block, :, 0:4 * SLOT] = moved
            elif group == groups - 1:
                s_out[block, :, 4 * SLOT:] = moved
            else:
                s_in[block, :, 4 * SLOT * (group - 1):4 * SLOT * group] = moved

    load_s.wait()
    reorder(core)

    pl.semaphore_wait(barrier, 1 + 2 * has[0].astype(jnp.int32) + 2 * has[1].astype(jnp.int32))

    def start_message(way, j, half):
        lane = pl.ds(half * width, width)
        col = other if j == 0 else core
        return pltpu.make_async_remote_copy(send_0.at[way, j, :, lane], recv_0.at[1 - way, core, :, lane], send0_sem.at[way, j, half],
                                            recv0_sem.at[1 - way, core, half], device_id=(col, near[way]), device_id_type=MESH)

    def coef_message(way, j):
        col = other if j == 0 else core
        return pltpu.make_async_remote_copy(c_own.at[systems[j]], c_nbr.at[1 - way, core], csend.at[way, j], crecv.at[1 - way, core],
                                            device_id=(col, near[way]), device_id_type=MESH)

    for half in range(HALVES):
        for way in range(2):
            @pl.when(has[way])
            def _():
                for j in range(2):
                    start_message(way, j, half).start()
                    if half == 0:
                        coef_message(way, j).start()

    def swap(src, dst, index):
        return pltpu.make_async_remote_copy(src, dst, side_send.at[index], side_recv.at[index], device_id={"col": other}, device_id_type=MESH)

    swaps = [
        swap(c_hbm.at[1 - sys], c_raw.at[core], 0),
        swap(f_hbm.at[1 - sys], res.at[:, pl.ds(mine, SUB), :], 1),
        swap(u_hbm.at[1 - sys], cor.at[:, pl.ds(mine, SUB), :], 2),
        swap(s_hbm.at[1 - sys], s_raw.at[core], 3),
    ]
    for item in swaps:
        item.start()

    for way in range(2):
        @pl.when(jnp.logical_not(has[way]))
        def _():
            recv_0[way] = jnp.zeros(recv_0.shape[1:], F32)
            c_nbr[way] = jnp.zeros(c_nbr.shape[1:], F32)
            for rnd in range(SWEEPS - 1):
                recv_f[rnd, way] = jnp.zeros(recv_f.shape[2:], F32)
                recv_b[rnd, way] = jnp.zeros(recv_b.shape[2:], BF16)

    load_c_raw.wait()
    swaps[0].wait()
    for x in range(SUB):
        for block in range(2):
            c_wide[x, SUB * block:SUB * (block + 1), :] = column(c_raw, (block,), x)
    cell = lax.broadcasted_iota(jnp.int32, (BAND, LANES), 0)
    for x in range(SUB):
        own = c_wide[x]
        lo = 0.5 * (own + pltpu.roll(own, 1, 0))
        hi = 0.5 * (own + pltpu.roll(own, BAND - 1, 0))
        total = jnp.where(cell == 0, own, lo) + jnp.where(cell == BAND - 1, own, hi)
        face_lo[x] = jnp.where(cell == 0, 0.0, lo)
        face_hi[x] = jnp.where(cell == BAND - 1, 0.0, hi)
        if x > 0:
            low_x = 0.5 * (c_wide[x - 1] + own)
            face_x[x] = low_x
            total = total + low_x
        if x < SUB - 1:
            total = total + 0.5 * (own + c_wide[x + 1])
        diag[x] = total

    def neighbourless(x, lanes, static=False):
        here = cor[x, :, lanes]
        flux = diag[x] * here - face_lo[x] * pltpu.roll(here, 1, 0) - face_hi[x] * pltpu.roll(here, BAND - 1, 0)
        if not static or x > 0:
            flux = flux - face_x[x] * cor[x - 1, :, lanes]
        if not static or x < SUB - 1:
            flux = flux - face_x[x + 1] * cor[x + 1, :, lanes]
        return flux

    def put(window, place, lanes, values):
        low = values.astype(BF16)
        at = pl.ds(place * SLOT, SLOT) if isinstance(place, int) else pl.ds(pl.multiple_of(place * SLOT, SLOT), SLOT)
        window[0, at, lanes] = low[0:SLOT]
        window[1, at, lanes] = low[BAND - SLOT:BAND]

    def message(rnd, way, half):
        lane = pl.ds(half * width, width)
        to = (other, near[way])
        return (
            pltpu.make_async_remote_copy(send_f.at[rnd, way, :, :, lane], recv_f.at[rnd, 1 - way, :, :, lane], fsend.at[rnd, way, half],
                                         frecv.at[rnd, 1 - way, half], device_id=to, device_id_type=MESH),
            pltpu.make_async_remote_copy(send_b.at[rnd, way, :, lane], recv_b.at[rnd, 1 - way, :, lane], bsend.at[rnd, way, half],
                                         brecv.at[rnd, 1 - way, half], device_id=to, device_id_type=MESH),
        )

    def update_edges(omega, half, rnd=None):
        for way in range(2):
            x, y = EDGE_ROW[way], SECOND_ROW[way]
            for lanes in lanes_of(half):
                first = res[x, :, lanes] - omega * neighbourless(x, lanes, True)
                second = res[y, :, lanes] - omega * neighbourless(y, lanes, True)
                res[x, :, lanes] = first
                res[y, :, lanes] = second
                if rnd is not None:
                    send_f[rnd, way, 0, :, lanes] = cor[x, :, lanes]
                    send_f[rnd, way, 1, :, lanes] = first
                    send_b[rnd, way, :, lanes] = second.astype(BF16)
            if rnd is not None:
                @pl.when(has[way])
                def _():
                    for copy in message(rnd, way, half):
                        copy.start()

    def update_inner(omega):
        def body(x, carry):
            for lanes in all_lanes:
                new = res[x, :, lanes] - omega * neighbourless(x, lanes)
                res[x, :, lanes] = new
                put(w_in, x - 2, lanes, new)
            return carry
        lax.fori_loop(2, SUB - 2, body, 0)
        for way in range(2):
            for lanes in all_lanes:
                put(w_out, PLACES[way][3], lanes, res[SECOND_ROW[way], :, lanes])

    def presolve():
        for block in range(2):
            for part in range(0, CELLS, CHUNK):
                pre[block, part:part + CHUNK] = jnp.dot(s_in[block, part:part + CHUNK], w_in[block], preferred_element_type=F32)

    def take_edges(rnd, half, omega):
        for way in range(2):
            @pl.when(has[way])
            def _():
                if rnd == 0:
                    for block in range(2):
                        lane = pl.ds(half * width, width)
                        pltpu.make_async_remote_copy(send_0.at[way, block, :, lane], recv_0.at[way, block, :, lane], send0_sem.at[way, block, half],
                                                     recv0_sem.at[way, block, half], device_id=(other, near[way]), device_id_type=MESH).wait_recv()
                else:
                    for copy in message(rnd - 1, 1 - way, half):
                        copy.wait_recv()
        for way in range(2):
            x = EDGE_ROW[way]
            face = face_x[0] if way == 0 else face_x[SUB]
            for lanes in lanes_of(half):
                if rnd == 0:
                    z_far, r_far, r_beyond = [jnp.concatenate([recv_0[way, block, SUB * i:SUB * (i + 1), lanes] for block in range(2)], axis=0) for i in range(3)]
                    none = jnp.zeros((SUB - 8, LANES), F32)
                    z_beyond = jnp.concatenate([none] + [recv_0[way, block, 3 * SUB:FIRST, lanes] for block in range(2)] + [none], axis=0)
                    side = cross[way, 0] * (z_far - pltpu.roll(z_far, 1, 0))
                    r_far = r_far - side + pltpu.roll(side, BAND - 1, 0)
                    side = cross[way, 1] * (z_beyond - pltpu.roll(z_beyond, 1, 0))
                    r_beyond = r_beyond - side + pltpu.roll(side, BAND - 1, 0)
                else:
                    z_far = recv_f[rnd - 1, way, 0, :, lanes]
                    r_far = recv_f[rnd - 1, way, 1, :, lanes]
                    r_beyond = recv_b[rnd - 1, way, :, lanes]
                flux = omega * face * (cor[x, :, lanes] - z_far)
                new = res[x, :, lanes] - flux
                res[x, :, lanes] = new
                put(w_out, PLACES[way][0], lanes, r_beyond)
                put(w_out, PLACES[way][1], lanes, r_far + flux)
                put(w_out, PLACES[way][2], lanes, new)

    def solve(block, part, lanes):
        return pre[block, part:part + CHUNK, lanes] + jnp.dot(s_out[block, part:part + CHUNK], w_out[block, :, lanes], preferred_element_type=F32)

    def rows_of(part):
        return ROW_ORDER[part // SUB:(part + CHUNK) // SUB]

    for load in (load_f, load_u):
        load.wait()
    for item in swaps[1:3]:
        item.wait()
    for half in range(HALVES):
        update_edges(1.0, half)
    update_inner(1.0)
    for block in range(2):
        for x in range(SUB):
            app[block, x] = cor[x, SUB * block:SUB * (block + 1), :]
    swaps[3].wait()
    reorder(other)
    presolve()

    for way in range(2):
        @pl.when(has[way])
        def _():
            for block in range(2):
                pltpu.make_async_remote_copy(c_own.at[block], c_nbr.at[way, block], csend.at[way, block], crecv.at[way, block],
                                             device_id=(other, near[way]), device_id_type=MESH).wait_recv()
        own = c_wide[EDGE_ROW[way]]
        beyond = [jnp.concatenate([column(c_nbr, (way, block), x) for block in range(2)], axis=0) for x in (EDGE_ROW[1 - way], SECOND_ROW[1 - way])]
        face_x[0 if way == 0 else SUB] = 0.5 * (own + jnp.where(has[way], beyond[0], own))
        for i in range(2):
            cross[way, i] = jnp.where(cell == SUB, 0.5 * (beyond[i] + pltpu.roll(beyond[i], 1, 0)), 0.0)

    omega = om_ref[sys]
    for sweep in range(SWEEPS - 1):
        before = 1.0 if sweep == 0 else omega
        for half in range(HALVES):
            lanes = slice(half * width, (half + 1) * width)
            take_edges(sweep, half, before)
            for block in range(2):
                part = solve(block, 0, lanes)
                for i, x in enumerate(EDGE_ROWS):
                    cor[x, SUB * block:SUB * (block + 1), lanes] = part[SUB * i:SUB * (i + 1)]
            update_edges(omega, half, sweep)
        for block in range(2):
            for x in EDGE_ROWS:
                app[block, x] = app[block, x] + omega * cor[x, SUB * block:SUB * (block + 1), :]
            for at in range(EDGE_CELLS, CELLS, CHUNK):
                part = solve(block, at, slice(0, RHS))
                for i, x in enumerate(rows_of(at)):
                    piece = part[SUB * i:SUB * (i + 1)]
                    cor[x, SUB * block:SUB * (block + 1), :] = piece
                    app[block, x] = app[block, x] + omega * piece
        update_inner(omega)
        presolve()

    def back(half):
        lane = pl.ds(half * width, width)
        return pltpu.make_async_remote_copy(fin.at[:, :, lane], out_ref.at[sys, :, :, lane], back_send.at[half], back_recv.at[half],
                                            device_id={"col": other}, device_id_type=MESH)

    for half in range(HALVES):
        lanes = slice(half * width, (half + 1) * width)
        take_edges(SWEEPS - 1, half, omega)
        for at in range(0, CELLS, CHUNK):
            part = solve(other, at, lanes)
            for i, x in enumerate(rows_of(at)):
                fin[x, :, lanes] = app[other, x, :, lanes] + omega * part[SUB * i:SUB * (i + 1)]
        back(half).start()
    for at in range(0, CELLS, CHUNK):
        part = solve(core, at, slice(0, RHS))
        for i, x in enumerate(rows_of(at)):
            out_ref[sys, x] = app[core, x] + omega * part[SUB * i:SUB * (i + 1)]

    for half in range(HALVES):
        back(half).wait_send()
        lane = pl.ds(half * width, width)
        pltpu.make_async_remote_copy(fin.at[:, :, lane], out_ref.at[1 - sys, :, :, lane], back_send.at[half], back_recv.at[half],
                                     device_id={"col": other}, device_id_type=MESH).wait_recv()
    for way in range(2):
        @pl.when(has[way])
        def _():
            for j in range(2):
                coef_message(way, j).wait_send()
            for half in range(HALVES):
                for j in range(2):
                    start_message(way, j, half).wait_send()
                for rnd in range(SWEEPS - 1):
                    for copy in message(rnd, way, half):
                        copy.wait_send()


def solution(mesh):
    rows = mesh.shape["row"]
    grid_spec = P(None, "row", "col", None)

    def local_sweeps(forcing, init_guess, cell_coef, solve_rows, relax_factor):
        solve_mat = jnp.swapaxes(solve_rows.reshape(2, CELLS, EXT * EXT), 1, 2)
        any_space = pl.BlockSpec(memory_space=pl.ANY)
        rounds = SWEEPS - 1
        wide = (SUB, BAND, LANES)
        dma = pltpu.SemaphoreType.DMA
        held = [pltpu.with_memory_space_constraint(v, pltpu.HBM) for v in (forcing, init_guess, cell_coef, solve_mat, relax_factor)]
        return pl.pallas_call(
            functools.partial(kernel, rows),
            out_shape=jax.ShapeDtypeStruct(forcing.shape, F32),
            in_specs=[any_space] * 4 + [pl.BlockSpec(memory_space=pltpu.SMEM)],
            out_specs=pl.BlockSpec(memory_space=pltpu.VMEM),
            scratch_shapes=[
                pltpu.VMEM((SUB, BAND, RHS), F32),
                pltpu.VMEM((SUB, BAND, RHS), F32),
                pltpu.VMEM((2, SUB, SUB, RHS), F32),
                pltpu.VMEM((SUB, SUB, RHS), F32),
                pltpu.VMEM((2, CELLS, RHS), F32),
                pltpu.VMEM((2, EXT * EXT, CELLS), BF16),
                pltpu.VMEM((2, CELLS, OUTER * SLOT), BF16),
                pltpu.VMEM((2, CELLS, INNER * SLOT), BF16),
                pltpu.VMEM((2, OUTER * SLOT, RHS), BF16),
                pltpu.VMEM((2, INNER * SLOT, RHS), BF16),
                pltpu.VMEM((2, SUB, SUB), F32),
                pltpu.VMEM((2, SUB, SUB), F32),
                pltpu.VMEM((2, 2, SUB, SUB), F32),
                pltpu.VMEM(wide, F32),
                pltpu.VMEM((2, SUB, SUB, LANES), F32),
                pltpu.VMEM((SUB + 1, BAND, LANES), F32),
                pltpu.VMEM(wide, F32),
                pltpu.VMEM(wide, F32),
                pltpu.VMEM((2, 2, BAND, LANES), F32),
                pltpu.VMEM(wide, F32),
                pltpu.VMEM((2, 2, 3, SUB, RHS), F32),
                pltpu.VMEM((2, 2, 2, SUB, RHS), F32),
                pltpu.VMEM((2, 2, FIRST, RHS), F32),
                pltpu.VMEM((2, 2, FIRST, RHS), F32),
                pltpu.VMEM((rounds, 2, 2, BAND, RHS), F32),
                pltpu.VMEM((rounds, 2, BAND, RHS), BF16),
                pltpu.VMEM((rounds, 2, 2, BAND, RHS), F32),
                pltpu.VMEM((rounds, 2, BAND, RHS), BF16),
                dma((5,)), dma((2, 2, 2)), dma((4,)), dma((4,)), dma((2, 2)), dma((2, 2)), dma((2, 2, HALVES)), dma((2, 2, HALVES)),
                dma((rounds, 2, HALVES)), dma((rounds, 2, HALVES)), dma((rounds, 2, HALVES)), dma((rounds, 2, HALVES)),
                dma((HALVES,)), dma((HALVES,)),
            ],
            compiler_params=pltpu.CompilerParams(collective_id=0, has_side_effects=True, vmem_limit_bytes=40 * 1024 * 1024),
        )(*held)

    return jax.shard_map(local_sweeps, mesh=mesh, in_specs=(grid_spec, grid_spec, P(None, "row", "col"), P(None, "row", "col", None, None), P(None)), out_specs=grid_spec, check_vma=False)
```

```python
import functools

import jax
import jax.numpy as jnp
from jax import lax
from jax.experimental import pallas as pl
from jax.experimental.pallas import tpu as pltpu
from jax.sharding import PartitionSpec as P

SWEEPS = 4
SUB = 24
MARGIN = 2
EXT = SUB + 2 * MARGIN
BAND = 2 * SUB
SLOT = 32
OUTER = 8
INNER = EXT - OUTER
LANES = 128
RHS = 2 * LANES
HALVES = 2
F32 = jnp.float32
BF16 = jnp.bfloat16
MESH = pl.DeviceIdType.MESH

EDGE_ROWS = (0, 1, 2, SUB - 3, SUB - 2, SUB - 1)
ROW_ORDER = EDGE_ROWS + tuple(range(3, SUB - 3))
EDGE_CELLS = SUB * len(EDGE_ROWS)
CELLS = SUB * SUB
CHUNK = EDGE_CELLS
EDGE_ROW = (0, SUB - 1)
SECOND_ROW = (1, SUB - 2)
PLACES = ((0, 1, 2, 3), (7, 6, 5, 4))
FIRST = 80


def kernel(rows, f_hbm, u_hbm, c_hbm, s_hbm, om_ref, out_ref, res, cor, app, fin, pre, s_raw, s_out, s_in, w_out, w_in, c_own, c_raw, c_nbr,
           c_wide, c_part, face_x, face_lo, face_hi, cross, diag, u_edge, f_edge, f_swap, u_swap, so_swap, si_swap, w_fin, fin_recv, send_0, recv_0, send_f, send_b, recv_f, recv_b,
           loc_sem, s_sem, edge_sem, side_send, side_recv, csend, crecv, send0_sem, recv0_sem, zsend, zrecv, fsend, frecv, bsend, brecv, back_send, back_recv):
    core = lax.axis_index("col")
    row = lax.axis_index("row")
    other = 1 - core
    sys = lax.rem(core + row, 2)
    systems = (sys, 1 - sys)
    has = (row > 0, row < rows - 1)
    near = (jnp.maximum(row - 1, 0), jnp.minimum(row + 1, rows - 1))
    mine = pl.multiple_of(core * SUB, 8)
    width = RHS // HALVES

    def lanes_of(half):
        return [slice(half * width + LANES * i, half * width + LANES * (i + 1)) for i in range(width // LANES)]

    all_lanes = [slice(LANES * i, LANES * (i + 1)) for i in range(RHS // LANES)]

    load_c = pltpu.make_async_copy(c_hbm, c_own, loc_sem.at[0])
    load_c.start()
    edge_loads = []
    for j in range(2):
        for way in range(2):
            edge_loads.append(pltpu.make_async_copy(u_hbm.at[systems[j], (SUB - 3) * way:(SUB - 3) * way + 3], u_edge.at[j, way], edge_sem.at[j, way, 0]))
            edge_loads.append(pltpu.make_async_copy(f_hbm.at[systems[j], (SUB - 2) * way:(SUB - 2) * way + 2], f_edge.at[j, way], edge_sem.at[j, way, 1]))
    for load in edge_loads:
        load.start()
    load_c_raw = pltpu.make_async_copy(c_hbm.at[sys], c_raw.at[core], loc_sem.at[4])
    load_s = [pltpu.make_async_copy(s_hbm.at[systems[j]], s_raw.at[j], s_sem.at[j]) for j in range(2)]
    load_f = pltpu.make_async_copy(f_hbm.at[sys], res.at[:, pl.ds(mine, SUB), :], loc_sem.at[1])
    load_u = pltpu.make_async_copy(u_hbm.at[sys], cor.at[:, pl.ds(mine, SUB), :], loc_sem.at[2])
    load_f_swap = pltpu.make_async_copy(f_hbm.at[1 - sys], f_swap, loc_sem.at[3])
    load_u_swap = pltpu.make_async_copy(u_hbm.at[1 - sys], u_swap, loc_sem.at[5])
    for load in (load_c_raw, load_s[1], load_f_swap, load_u_swap, load_s[0], load_f, load_u):
        load.start()

    barrier = pltpu.get_barrier_semaphore()
    for way in range(2):
        @pl.when(has[way])
        def _():
            for col in range(2):
                pl.semaphore_signal(barrier, inc=1, device_id=(col, near[way]), device_id_type=MESH)
    pl.semaphore_signal(barrier, inc=1, device_id={"col": other}, device_id_type=MESH)

    eye = lax.broadcasted_iota(jnp.int32, (SUB, SUB), 0) == lax.broadcasted_iota(jnp.int32, (SUB, SUB), 1)

    def column(ref, lead, x):
        line = jnp.broadcast_to(ref[lead + (pl.ds(x, 1), slice(None))], (SUB, SUB))
        return jnp.broadcast_to(jnp.sum(jnp.where(eye, line, 0.0), axis=1, keepdims=True), (SUB, LANES))

    load_c.wait()
    for j in range(2):
        for x in EDGE_ROWS:
            c_part[j, x] = column(c_own, (systems[j],), x)
    for load in edge_loads:
        load.wait()
    spot = lax.broadcasted_iota(jnp.int32, (SUB, LANES), 0)
    for j in range(2):
        for way in range(2):
            step = 1 if way == 0 else -1
            place = (0, 1, 2) if way == 0 else (2, 1, 0)
            into = (0, 1) if way == 0 else (1, 0)
            at = [EDGE_ROW[way] + step * i for i in range(3)]
            c = [c_part[j, x] for x in at]
            link = [0.5 * (c[0] + c[1]), 0.5 * (c[1] + c[2])]
            for i in range(2):
                lo = jnp.where(spot == 0, 0.0, 0.5 * (c[i] + pltpu.roll(c[i], 1, 0)))
                hi = jnp.where(spot == SUB - 1, 0.0, 0.5 * (c[i] + pltpu.roll(c[i], SUB - 1, 0)))
                wall = jnp.where((spot == 0) & (core == 0) | (spot == SUB - 1) & (core == 1), c[i], 0.0)
                total = lo + hi + wall + link[i]
                if i == 1:
                    total = total + link[0]
                for lanes in all_lanes:
                    u = [u_edge[j, way, place[n], :, lanes] for n in range(3)]
                    flux = total * u[i] - lo * pltpu.roll(u[i], 1, 0) - hi * pltpu.roll(u[i], SUB - 1, 0) - link[i] * u[i + 1]
                    if i == 1:
                        flux = flux - link[0] * u[0]
                    send_0[way, j, SUB * (i + 1):SUB * (i + 2), lanes] = f_edge[j, way, into[i], :, lanes] - flux
                    if i == 0:
                        send_0[way, j, 0:SUB, lanes] = u[0]
            tile = jnp.where(core == 0, u_edge[j, way, place[1], SUB - 8:SUB, :], u_edge[j, way, place[1], 0:8, :])
            send_0[way, j, 3 * SUB:FIRST, :] = tile

    source = lax.broadcasted_iota(jnp.int32, (4 * EXT, 4 * SLOT), 0)
    target = lax.broadcasted_iota(jnp.int32, (4 * EXT, 4 * SLOT), 1)
    ext_x = lax.shift_right_logical(source * 2341, 16)
    ext_y = source - EXT * ext_x

    shift = (SUB - (BAND - SLOT)) * core - MARGIN
    inside = ext_y + SUB * core - MARGIN
    hit = (target == ext_x * SLOT + ext_y + shift) & (inside >= 0) & (inside < BAND)
    pick = jnp.where(hit, 1.0, 0.0).astype(BF16)

    def reorder(j, outer, inner):
        groups = EXT // 4
        for group in range(groups):
            moved = lax.dot_general(s_raw[j, 4 * EXT * group:4 * EXT * (group + 1), :], pick, (((0,), (0,)), ((), ())), preferred_element_type=F32)
            cut = 3 * SUB
            moved = jnp.concatenate([moved[:cut], moved[-cut:], moved[cut:-cut]], axis=0).astype(BF16)
            if group == 0:
                outer[:, 0:4 * SLOT] = moved
            elif group == groups - 1:
                outer[:, 4 * SLOT:] = moved
            else:
                inner[:, 4 * SLOT * (group - 1):4 * SLOT * group] = moved

    load_s[1].wait()
    reorder(1, so_swap, si_swap)
    load_s[0].wait()
    reorder(0, s_out.at[core], s_in.at[core])
    load_f_swap.wait()
    load_u_swap.wait()

    pl.semaphore_wait(barrier, 1 + 2 * has[0].astype(jnp.int32) + 2 * has[1].astype(jnp.int32))

    def start_message(way, col, half):
        lane = pl.ds(half * width, width)
        j = other if col == 0 else core
        return pltpu.make_async_remote_copy(send_0.at[way, j, :, lane], recv_0.at[1 - way, core, :, lane], send0_sem.at[way, col, half],
                                            recv0_sem.at[1 - way, core, half], device_id=(col, near[way]), device_id_type=MESH)

    def coef_message(way, col):
        there = lax.rem(sys + (other if col == 0 else core), 2)
        tile = pl.ds((SUB - 8) * way, 8)
        return pltpu.make_async_remote_copy(c_own.at[there, tile], c_nbr.at[1 - way, core], csend.at[way, col], crecv.at[1 - way, core],
                                            device_id=(col, near[way]), device_id_type=MESH)

    for way in range(2):
        @pl.when(has[way])
        def _():
            for col in (1, 0):
                coef_message(way, col).start()
    for half in range(HALVES):
        for way in range(2):
            @pl.when(has[way])
            def _():
                for col in (1, 0):
                    start_message(way, col, half).start()

    def swap(src, dst, index):
        return pltpu.make_async_remote_copy(src, dst, side_send.at[index], side_recv.at[index], device_id={"col": other}, device_id_type=MESH)

    swaps = [
        swap(c_own.at[1 - sys], c_raw.at[core], 0),
        swap(u_swap, cor.at[:, pl.ds(mine, SUB), :], 1),
        swap(f_swap, res.at[:, pl.ds(mine, SUB), :], 2),
        swap(si_swap, s_in.at[core], 3),
        swap(so_swap, s_out.at[core], 4),
    ]
    for item in swaps:
        item.start()

    for way in range(2):
        @pl.when(jnp.logical_not(has[way]))
        def _():
            recv_0[way] = jnp.zeros(recv_0.shape[1:], F32)
            c_nbr[way] = jnp.zeros(c_nbr.shape[1:], F32)
            for rnd in range(SWEEPS - 1):
                recv_f[rnd, way] = jnp.zeros(recv_f.shape[2:], F32)
                recv_b[rnd, way] = jnp.zeros(recv_b.shape[2:], BF16)

    load_c_raw.wait()
    swaps[0].wait()
    for x in range(SUB):
        for block in range(2):
            c_wide[x, SUB * block:SUB * (block + 1), :] = column(c_raw, (block,), x)
    cell = lax.broadcasted_iota(jnp.int32, (BAND, LANES), 0)
    for x in range(SUB):
        own = c_wide[x]
        lo = 0.5 * (own + pltpu.roll(own, 1, 0))
        hi = 0.5 * (own + pltpu.roll(own, BAND - 1, 0))
        total = jnp.where(cell == 0, own, lo) + jnp.where(cell == BAND - 1, own, hi)
        face_lo[x] = jnp.where(cell == 0, 0.0, lo)
        face_hi[x] = jnp.where(cell == BAND - 1, 0.0, hi)
        if x > 0:
            low_x = 0.5 * (c_wide[x - 1] + own)
            face_x[x] = low_x
            total = total + low_x
        if x < SUB - 1:
            total = total + 0.5 * (own + c_wide[x + 1])
        diag[x] = total

    def neighbourless(x, lanes, static=False):
        here = cor[x, :, lanes]
        flux = diag[x] * here - face_lo[x] * pltpu.roll(here, 1, 0) - face_hi[x] * pltpu.roll(here, BAND - 1, 0)
        if not static or x > 0:
            flux = flux - face_x[x] * cor[x - 1, :, lanes]
        if not static or x < SUB - 1:
            flux = flux - face_x[x + 1] * cor[x + 1, :, lanes]
        return flux

    def put(window, place, lanes, values):
        low = values.astype(BF16)
        at = pl.ds(place * SLOT, SLOT) if isinstance(place, int) else pl.ds(pl.multiple_of(place * SLOT, SLOT), SLOT)
        window[0, at, lanes] = low[0:SLOT]
        window[1, at, lanes] = low[BAND - SLOT:BAND]

    def message(rnd, way, half):
        lane = pl.ds(half * width, width)
        to = (other, near[way])
        return (
            pltpu.make_async_remote_copy(send_f.at[rnd, way, 0, :, lane], recv_f.at[rnd, 1 - way, 0, :, lane], zsend.at[rnd, way, half],
                                         zrecv.at[rnd, 1 - way, half], device_id=to, device_id_type=MESH),
            pltpu.make_async_remote_copy(send_f.at[rnd, way, 1, :, lane], recv_f.at[rnd, 1 - way, 1, :, lane], fsend.at[rnd, way, half],
                                         frecv.at[rnd, 1 - way, half], device_id=to, device_id_type=MESH),
            pltpu.make_async_remote_copy(send_b.at[rnd, way, :, lane], recv_b.at[rnd, 1 - way, :, lane], bsend.at[rnd, way, half],
                                         brecv.at[rnd, 1 - way, half], device_id=to, device_id_type=MESH),
        )

    def update_edges(omega, half, rnd=None):
        for way in range(2):
            x, y = EDGE_ROW[way], SECOND_ROW[way]
            for lanes in lanes_of(half):
                first = res[x, :, lanes] - omega * neighbourless(x, lanes, True)
                second = res[y, :, lanes] - omega * neighbourless(y, lanes, True)
                res[x, :, lanes] = first
                res[y, :, lanes] = second
                if rnd is not None:
                    send_f[rnd, way, 1, :, lanes] = first
                    send_b[rnd, way, :, lanes] = second.astype(BF16)
            if rnd is not None:
                @pl.when(has[way])
                def _():
                    for copy in message(rnd, way, half)[1:]:
                        copy.start()

    def update_inner(omega):
        def body(x, carry):
            for lanes in all_lanes:
                new = res[x, :, lanes] - omega * neighbourless(x, lanes)
                res[x, :, lanes] = new
                put(w_in, x - 2, lanes, new)
            return carry
        lax.fori_loop(2, SUB - 2, body, 0)
        for way in range(2):
            for lanes in all_lanes:
                put(w_out, PLACES[way][3], lanes, res[SECOND_ROW[way], :, lanes])

    def presolve():
        for block in range(2):
            for part in range(0, CELLS, CHUNK):
                pre[block, part:part + CHUNK] = jnp.dot(s_in[block, part:part + CHUNK], w_in[block], preferred_element_type=F32)

    def take_edges(rnd, half, omega):
        for way in range(2):
            @pl.when(has[way])
            def _():
                if rnd == 0:
                    for block in range(2):
                        lane = pl.ds(half * width, width)
                        pltpu.make_async_remote_copy(send_0.at[way, block, :, lane], recv_0.at[way, block, :, lane], send0_sem.at[way, block, half],
                                                     recv0_sem.at[way, block, half], device_id=(other, near[way]), device_id_type=MESH).wait_recv()
                else:
                    for copy in message(rnd - 1, 1 - way, half):
                        copy.wait_recv()
        for way in range(2):
            x = EDGE_ROW[way]
            face = face_x[0] if way == 0 else face_x[SUB]
            for lanes in lanes_of(half):
                if rnd == 0:
                    z_far, r_far, r_beyond = [jnp.concatenate([recv_0[way, block, SUB * i:SUB * (i + 1), lanes] for block in range(2)], axis=0) for i in range(3)]
                    none = jnp.zeros((SUB - 8, LANES), F32)
                    z_beyond = jnp.concatenate([none] + [recv_0[way, block, 3 * SUB:FIRST, lanes] for block in range(2)] + [none], axis=0)
                    side = cross[way, 0] * (z_far - pltpu.roll(z_far, 1, 0))
                    r_far = r_far - side + pltpu.roll(side, BAND - 1, 0)
                    side = cross[way, 1] * (z_beyond - pltpu.roll(z_beyond, 1, 0))
                    r_beyond = r_beyond - side + pltpu.roll(side, BAND - 1, 0)
                else:
                    z_far = recv_f[rnd - 1, way, 0, :, lanes]
                    r_far = recv_f[rnd - 1, way, 1, :, lanes]
                    r_beyond = recv_b[rnd - 1, way, :, lanes]
                flux = omega * face * (cor[x, :, lanes] - z_far)
                new = res[x, :, lanes] - flux
                res[x, :, lanes] = new
                put(w_out, PLACES[way][0], lanes, r_beyond)
                put(w_out, PLACES[way][1], lanes, r_far + flux)
                put(w_out, PLACES[way][2], lanes, new)

    def solve(block, part, lanes):
        return pre[block, part:part + CHUNK, lanes] + jnp.dot(s_out[block, part:part + CHUNK], w_out[block, :, lanes], preferred_element_type=F32)

    def rows_of(part):
        return ROW_ORDER[part // SUB:(part + CHUNK) // SUB]

    for load in (load_f, load_u):
        load.wait()
    for item in swaps[1:3]:
        item.wait()
    for half in range(HALVES):
        update_edges(1.0, half)
    update_inner(1.0)
    for block in range(2):
        for x in range(SUB):
            app[block, x] = cor[x, SUB * block:SUB * (block + 1), :]
    for item in swaps[3:]:
        item.wait()
    presolve()

    for way in range(2):
        @pl.when(has[way])
        def _():
            for block in range(2):
                pltpu.make_async_remote_copy(c_own.at[block, 0:8], c_nbr.at[way, block], csend.at[way, block], crecv.at[way, block],
                                             device_id=(other, near[way]), device_id_type=MESH).wait_recv()
        own = c_wide[EDGE_ROW[way]]
        beyond = [jnp.concatenate([column(c_nbr, (way, block), x) for block in range(2)], axis=0) for x in ((7, 6) if way == 0 else (0, 1))]
        face_x[0 if way == 0 else SUB] = 0.5 * (own + jnp.where(has[way], beyond[0], own))
        for i in range(2):
            cross[way, i] = jnp.where(cell == SUB, 0.5 * (beyond[i] + pltpu.roll(beyond[i], 1, 0)), 0.0)

    omega = om_ref[sys]
    for sweep in range(SWEEPS - 1):
        before = 1.0 if sweep == 0 else omega
        for half in range(HALVES):
            lanes = slice(half * width, (half + 1) * width)
            take_edges(sweep, half, before)
            for block in range(2):
                part = solve(block, 0, lanes)
                for i, x in enumerate(EDGE_ROWS):
                    cor[x, SUB * block:SUB * (block + 1), lanes] = part[SUB * i:SUB * (i + 1)]
                    if x in EDGE_ROW:
                        send_f[sweep, EDGE_ROW.index(x), 0, SUB * block:SUB * (block + 1), lanes] = part[SUB * i:SUB * (i + 1)]
            for way in range(2):
                @pl.when(has[way])
                def _():
                    message(sweep, way, half)[0].start()
            update_edges(omega, half, sweep)
        for block in range(2):
            for x in EDGE_ROWS:
                app[block, x] = app[block, x] + omega * cor[x, SUB * block:SUB * (block + 1), :]
            for at in range(EDGE_CELLS, CELLS, CHUNK):
                part = solve(block, at, slice(0, RHS))
                for i, x in enumerate(rows_of(at)):
                    piece = part[SUB * i:SUB * (i + 1)]
                    cor[x, SUB * block:SUB * (block + 1), :] = piece
                    app[block, x] = app[block, x] + omega * piece
        update_inner(omega)
        presolve()

    for at in range(0, CELLS, CHUNK):
        for i, x in enumerate(rows_of(at)):
            here = slice(at + SUB * i, at + SUB * (i + 1))
            fin[x] = app[other, x] + omega * pre[other, here]
    early = pltpu.make_async_remote_copy(fin, fin_recv, back_send.at[HALVES], back_recv.at[HALVES], device_id={"col": other}, device_id_type=MESH)
    early.start()

    def back(half):
        lane = pl.ds(half * width, width)
        return pltpu.make_async_remote_copy(w_out.at[other, :, lane], w_fin.at[:, lane], back_send.at[half], back_recv.at[half],
                                            device_id={"col": other}, device_id_type=MESH)

    def finish_own(half):
        lanes = slice(half * width, (half + 1) * width)
        for at in range(0, CELLS, CHUNK):
            part = solve(core, at, lanes)
            for i, x in enumerate(rows_of(at)):
                out_ref[sys, x, :, lanes] = app[core, x, :, lanes] + omega * part[SUB * i:SUB * (i + 1)]

    def finish_other(half):
        lanes = slice(half * width, (half + 1) * width)
        back(half).wait()
        for at in range(0, CELLS, CHUNK):
            part = jnp.dot(so_swap[at:at + CHUNK], w_fin[:, lanes], preferred_element_type=F32)
            for i, x in enumerate(rows_of(at)):
                out_ref[1 - sys, x, :, lanes] = fin_recv[x, :, lanes] + their_omega * part[SUB * i:SUB * (i + 1)]

    their_omega = om_ref[1 - sys]
    take_edges(SWEEPS - 1, 0, omega)
    back(0).start()
    take_edges(SWEEPS - 1, 1, omega)
    back(1).start()
    finish_own(0)
    finish_own(1)
    early.wait()
    finish_other(0)
    finish_other(1)
    for way in range(2):
        @pl.when(has[way])
        def _():
            for j in range(2):
                coef_message(way, j).wait_send()
            for half in range(HALVES):
                for j in range(2):
                    start_message(way, j, half).wait_send()
                for rnd in range(SWEEPS - 1):
                    for copy in message(rnd, way, half):
                        copy.wait_send()


def solution(mesh):
    rows = mesh.shape["row"]
    grid_spec = P(None, "row", "col", None)

    def local_sweeps(forcing, init_guess, cell_coef, solve_rows, relax_factor):
        solve_mat = jnp.swapaxes(solve_rows.reshape(2, CELLS, EXT * EXT), 1, 2)
        any_space = pl.BlockSpec(memory_space=pl.ANY)
        rounds = SWEEPS - 1
        wide = (SUB, BAND, LANES)
        dma = pltpu.SemaphoreType.DMA
        held = [pltpu.with_memory_space_constraint(v, pltpu.HBM) for v in (forcing, init_guess, cell_coef, solve_mat, relax_factor)]
        return pl.pallas_call(
            functools.partial(kernel, rows),
            out_shape=jax.ShapeDtypeStruct(forcing.shape, F32),
            in_specs=[any_space] * 4 + [pl.BlockSpec(memory_space=pltpu.SMEM)],
            out_specs=pl.BlockSpec(memory_space=pltpu.VMEM),
            scratch_shapes=[
                pltpu.VMEM((SUB, BAND, RHS), F32),
                pltpu.VMEM((SUB, BAND, RHS), F32),
                pltpu.VMEM((2, SUB, SUB, RHS), F32),
                pltpu.VMEM((SUB, SUB, RHS), F32),
                pltpu.VMEM((2, CELLS, RHS), F32),
                pltpu.VMEM((2, EXT * EXT, CELLS), BF16),
                pltpu.VMEM((2, CELLS, OUTER * SLOT), BF16),
                pltpu.VMEM((2, CELLS, INNER * SLOT), BF16),
                pltpu.VMEM((2, OUTER * SLOT, RHS), BF16),
                pltpu.VMEM((2, INNER * SLOT, RHS), BF16),
                pltpu.VMEM((2, SUB, SUB), F32),
                pltpu.VMEM((2, SUB, SUB), F32),
                pltpu.VMEM((2, 2, 8, SUB), F32),
                pltpu.VMEM(wide, F32),
                pltpu.VMEM((2, SUB, SUB, LANES), F32),
                pltpu.VMEM((SUB + 1, BAND, LANES), F32),
                pltpu.VMEM(wide, F32),
                pltpu.VMEM(wide, F32),
                pltpu.VMEM((2, 2, BAND, LANES), F32),
                pltpu.VMEM(wide, F32),
                pltpu.VMEM((2, 2, 3, SUB, RHS), F32),
                pltpu.VMEM((2, 2, 2, SUB, RHS), F32),
                pltpu.VMEM((SUB, SUB, RHS), F32),
                pltpu.VMEM((SUB, SUB, RHS), F32),
                pltpu.VMEM((CELLS, OUTER * SLOT), BF16),
                pltpu.VMEM((CELLS, INNER * SLOT), BF16),
                pltpu.VMEM((OUTER * SLOT, RHS), BF16),
                pltpu.VMEM((SUB, SUB, RHS), F32),
                pltpu.VMEM((2, 2, FIRST, RHS), F32),
                pltpu.VMEM((2, 2, FIRST, RHS), F32),
                pltpu.VMEM((rounds, 2, 2, BAND, RHS), F32),
                pltpu.VMEM((rounds, 2, BAND, RHS), BF16),
                pltpu.VMEM((rounds, 2, 2, BAND, RHS), F32),
                pltpu.VMEM((rounds, 2, BAND, RHS), BF16),
                dma((6,)), dma((2,)), dma((2, 2, 2)), dma((5,)), dma((5,)), dma((2, 2)), dma((2, 2)), dma((2, 2, HALVES)), dma((2, 2, HALVES)),
                *[dma((rounds, 2, HALVES))] * 6,
                dma((HALVES + 1,)), dma((HALVES + 1,)),
            ],
            compiler_params=pltpu.CompilerParams(collective_id=0, has_side_effects=True, vmem_limit_bytes=40 * 1024 * 1024),
        )(*held)

    return jax.shard_map(local_sweeps, mesh=mesh, in_specs=(grid_spec, grid_spec, P(None, "row", "col"), P(None, "row", "col", None, None), P(None)), out_specs=grid_spec, check_vma=False)
```

```python
import functools

import jax
import jax.numpy as jnp
from jax import lax
from jax.experimental import pallas as pl
from jax.experimental.pallas import tpu as pltpu
from jax.sharding import PartitionSpec as P

SWEEPS = 4
SUB = 24
MARGIN = 2
EXT = SUB + 2 * MARGIN
BAND = 2 * SUB
SLOT = 32
OUTER = 8
INNER = EXT - OUTER
LANES = 128
RHS = 2 * LANES
HALVES = 2
F32 = jnp.float32
BF16 = jnp.bfloat16
MESH = pl.DeviceIdType.MESH

EDGE_ROWS = (0, 1, 2, SUB - 3, SUB - 2, SUB - 1)
ROW_ORDER = EDGE_ROWS + tuple(range(3, SUB - 3))
EDGE_CELLS = SUB * len(EDGE_ROWS)
CELLS = SUB * SUB
CHUNK = EDGE_CELLS
EDGE_ROW = (0, SUB - 1)
SECOND_ROW = (1, SUB - 2)
PLACES = ((0, 1, 2, 3), (7, 6, 5, 4))
FIRST = 2 * SUB + 8


def kernel(rows, f_hbm, u_hbm, c_hbm, s_hbm, om_ref, out_ref, res, cor, app, fin, pre, s_raw, s_out, s_in, w_out, w_in, c_own, c_raw, c_nbr,
           c_wide, c_part, face_x, face_lo, face_hi, cross, diag, u_edge, f_edge, f_swap, u_swap, so_swap, si_swap, w_fin, fin_recv, send_0, recv_0, low_0, take_0, send_f, send_b, recv_f, recv_b,
           loc_sem, s_sem, edge_sem, side_send, side_recv, csend, crecv, send0_sem, recv0_sem, low0_sem, take0_sem, zsend, zrecv, fsend, frecv, bsend, brecv, back_send, back_recv):
    core = lax.axis_index("col")
    row = lax.axis_index("row")
    other = 1 - core
    sys = lax.rem(core + row, 2)
    systems = (sys, 1 - sys)
    has = (row > 0, row < rows - 1)
    near = (jnp.maximum(row - 1, 0), jnp.minimum(row + 1, rows - 1))
    slow = (lax.rem(row, 4) == 3).astype(jnp.int32)
    slow_first = (slow, 1 - slow)

    def present(way):
        there = row + 2 * way - 1
        return (there >= 0) & (there < rows)

    def neighbour(way):
        return jnp.clip(row + 2 * way - 1, 0, rows - 1)
    mine = pl.multiple_of(core * SUB, 8)
    width = RHS // HALVES

    def lanes_of(half):
        return [slice(half * width + LANES * i, half * width + LANES * (i + 1)) for i in range(width // LANES)]

    all_lanes = [slice(LANES * i, LANES * (i + 1)) for i in range(RHS // LANES)]

    load_c = pltpu.make_async_copy(c_hbm, c_own, loc_sem.at[0])
    load_c.start()
    edge_loads = []
    for j in range(2):
        for way in range(2):
            edge_loads.append(pltpu.make_async_copy(u_hbm.at[systems[j], (SUB - 3) * way:(SUB - 3) * way + 3], u_edge.at[j, way], edge_sem.at[j, way, 0]))
            edge_loads.append(pltpu.make_async_copy(f_hbm.at[systems[j], (SUB - 2) * way:(SUB - 2) * way + 2], f_edge.at[j, way], edge_sem.at[j, way, 1]))
    for load in edge_loads:
        load.start()
    load_c_raw = pltpu.make_async_copy(c_hbm.at[sys], c_raw.at[core], loc_sem.at[4])
    load_s = [pltpu.make_async_copy(s_hbm.at[systems[j]], s_raw.at[j], s_sem.at[j]) for j in range(2)]
    load_f = pltpu.make_async_copy(f_hbm.at[sys], res.at[:, pl.ds(mine, SUB), :], loc_sem.at[1])
    load_u = pltpu.make_async_copy(u_hbm.at[sys], cor.at[:, pl.ds(mine, SUB), :], loc_sem.at[2])
    load_f_swap = pltpu.make_async_copy(f_hbm.at[1 - sys], f_swap, loc_sem.at[3])
    load_u_swap = pltpu.make_async_copy(u_hbm.at[1 - sys], u_swap, loc_sem.at[5])
    for load in (load_c_raw, load_s[1], load_f_swap, load_u_swap, load_s[0], load_f, load_u):
        load.start()

    barrier = pltpu.get_barrier_semaphore()
    for way in range(2):
        @pl.when(has[way])
        def _():
            for col in range(2):
                pl.semaphore_signal(barrier, inc=1, device_id=(col, near[way]), device_id_type=MESH)
    pl.semaphore_signal(barrier, inc=1, device_id={"col": other}, device_id_type=MESH)

    eye = lax.broadcasted_iota(jnp.int32, (SUB, SUB), 0) == lax.broadcasted_iota(jnp.int32, (SUB, SUB), 1)

    def column(ref, lead, x):
        line = jnp.broadcast_to(ref[lead + (pl.ds(x, 1), slice(None))], (SUB, SUB))
        return jnp.broadcast_to(jnp.sum(jnp.where(eye, line, 0.0), axis=1, keepdims=True), (SUB, LANES))

    load_c.wait()
    for j in range(2):
        for x in EDGE_ROWS:
            c_part[j, x] = column(c_own, (systems[j],), x)
    for load in edge_loads:
        load.wait()
    spot = lax.broadcasted_iota(jnp.int32, (SUB, LANES), 0)
    tile_row = lax.broadcasted_iota(jnp.int32, (8, LANES), 0)
    for j in range(2):
        for way in range(2):
            step = 1 if way == 0 else -1
            place = (0, 1, 2) if way == 0 else (2, 1, 0)
            into = (0, 1) if way == 0 else (1, 0)
            at = [EDGE_ROW[way] + step * i for i in range(3)]
            c = [c_part[j, x] for x in at]
            link = [0.5 * (c[0] + c[1]), 0.5 * (c[1] + c[2])]
            for i in range(2):
                lo = jnp.where(spot == 0, 0.0, 0.5 * (c[i] + pltpu.roll(c[i], 1, 0)))
                hi = jnp.where(spot == SUB - 1, 0.0, 0.5 * (c[i] + pltpu.roll(c[i], SUB - 1, 0)))
                wall = jnp.where((spot == 0) & (core == 0) | (spot == SUB - 1) & (core == 1), c[i], 0.0)
                total = lo + hi + wall + link[i]
                if i == 1:
                    total = total + link[0]
                for lanes in all_lanes:
                    u = [u_edge[j, way, place[n], :, lanes] for n in range(3)]
                    flux = total * u[i] - lo * pltpu.roll(u[i], 1, 0) - hi * pltpu.roll(u[i], SUB - 1, 0) - link[i] * u[i + 1]
                    if i == 1:
                        flux = flux - link[0] * u[0]
                    part = f_edge[j, way, into[i], :, lanes] - flux
                    if i == 0:
                        send_0[way, j, 0:SUB, lanes] = u[0]
                        send_0[way, j, SUB:2 * SUB, lanes] = part
                    else:
                        low_0[way, j, :, lanes] = part.astype(BF16)
                        ends = [jnp.where(core == 0, v[SUB - 1:SUB], v[0:1]) for v in (u[1], part)]
                        send_0[way, j, 2 * SUB:FIRST, lanes] = jnp.where(tile_row == 0, ends[0], ends[1])

    source = lax.broadcasted_iota(jnp.int32, (4 * EXT, 4 * SLOT), 0)
    target = lax.broadcasted_iota(jnp.int32, (4 * EXT, 4 * SLOT), 1)
    ext_x = lax.shift_right_logical(source * 2341, 16)
    ext_y = source - EXT * ext_x

    shift = (SUB - (BAND - SLOT)) * core - MARGIN
    inside = ext_y + SUB * core - MARGIN
    hit = (target == ext_x * SLOT + ext_y + shift) & (inside >= 0) & (inside < BAND)
    pick = jnp.where(hit, 1.0, 0.0).astype(BF16)

    def reorder(j, outer, inner):
        groups = EXT // 4
        for group in range(groups):
            moved = lax.dot_general(s_raw[j, 4 * EXT * group:4 * EXT * (group + 1), :], pick, (((0,), (0,)), ((), ())), preferred_element_type=F32)
            cut = 3 * SUB
            moved = jnp.concatenate([moved[:cut], moved[-cut:], moved[cut:-cut]], axis=0).astype(BF16)
            if group == 0:
                outer[:, 0:4 * SLOT] = moved
            elif group == groups - 1:
                outer[:, 4 * SLOT:] = moved
            else:
                inner[:, 4 * SLOT * (group - 1):4 * SLOT * group] = moved

    load_s[1].wait()
    reorder(1, so_swap, si_swap)
    load_s[0].wait()
    reorder(0, s_out.at[core], s_in.at[core])
    load_f_swap.wait()
    load_u_swap.wait()

    pl.semaphore_wait(barrier, 1 + 2 * has[0].astype(jnp.int32) + 2 * has[1].astype(jnp.int32))

    def start_message(way, col, half):
        lane = pl.ds(half * width, width)
        j = other if col == 0 else core
        to = (col, near[way])
        return (
            pltpu.make_async_remote_copy(send_0.at[way, j, :, lane], recv_0.at[1 - way, core, :, lane], send0_sem.at[way, col, half],
                                         recv0_sem.at[1 - way, core, half], device_id=to, device_id_type=MESH),
            pltpu.make_async_remote_copy(low_0.at[way, j, :, lane], take_0.at[1 - way, core, :, lane], low0_sem.at[way, col, half],
                                         take0_sem.at[1 - way, core, half], device_id=to, device_id_type=MESH),
        )

    def coef_message(way, col):
        there = lax.rem(sys + (other if col == 0 else core), 2)
        tile = pl.ds((SUB - 8) * way, 8)
        return pltpu.make_async_remote_copy(c_own.at[there, tile], c_nbr.at[1 - way, core], csend.at[way, col], crecv.at[1 - way, core],
                                            device_id=(col, near[way]), device_id_type=MESH)

    for way in range(2):
        @pl.when(has[way])
        def _():
            for col in (1, 0):
                coef_message(way, col).start()
    for col in (1, 0):
        for half in range(HALVES):
            for way in range(2):
                @pl.when(has[way])
                def _():
                    for copy in start_message(way, col, half):
                        copy.start()

    def swap(src, dst, index):
        return pltpu.make_async_remote_copy(src, dst, side_send.at[index], side_recv.at[index], device_id={"col": other}, device_id_type=MESH)

    swaps = [
        swap(c_own.at[1 - sys], c_raw.at[core], 0),
        swap(u_swap, cor.at[:, pl.ds(mine, SUB), :], 1),
        swap(f_swap, res.at[:, pl.ds(mine, SUB), :], 2),
        swap(si_swap, s_in.at[core], 3),
        swap(so_swap, s_out.at[core], 4),
    ]
    for item in swaps:
        item.start()

    for way in range(2):
        @pl.when(jnp.logical_not(has[way]))
        def _():
            recv_0[way] = jnp.zeros(recv_0.shape[1:], F32)
            take_0[way] = jnp.zeros(take_0.shape[1:], BF16)
            c_nbr[way] = jnp.zeros(c_nbr.shape[1:], F32)
            for rnd in range(SWEEPS - 1):
                recv_f[rnd, way] = jnp.zeros(recv_f.shape[2:], F32)
                recv_b[rnd, way] = jnp.zeros(recv_b.shape[2:], BF16)

    load_c_raw.wait()
    swaps[0].wait()
    for x in range(SUB):
        for block in range(2):
            c_wide[x, SUB * block:SUB * (block + 1), :] = column(c_raw, (block,), x)
    cell = lax.broadcasted_iota(jnp.int32, (BAND, LANES), 0)
    for x in range(SUB):
        own = c_wide[x]
        lo = 0.5 * (own + pltpu.roll(own, 1, 0))
        hi = 0.5 * (own + pltpu.roll(own, BAND - 1, 0))
        total = jnp.where(cell == 0, own, lo) + jnp.where(cell == BAND - 1, own, hi)
        face_lo[x] = jnp.where(cell == 0, 0.0, lo)
        face_hi[x] = jnp.where(cell == BAND - 1, 0.0, hi)
        if x > 0:
            low_x = 0.5 * (c_wide[x - 1] + own)
            face_x[x] = low_x
            total = total + low_x
        if x < SUB - 1:
            total = total + 0.5 * (own + c_wide[x + 1])
        diag[x] = total

    def neighbourless(x, lanes, links):
        here = cor[x, :, lanes]
        flux = diag[x] * here - face_lo[x] * pltpu.roll(here, 1, 0) - face_hi[x] * pltpu.roll(here, BAND - 1, 0)
        for to, face in links:
            flux = flux - face_x[face] * cor[to, :, lanes]
        return flux

    def put(window, place, lanes, values):
        low = values.astype(BF16)
        at = pl.ds(place * SLOT, SLOT) if isinstance(place, int) else pl.ds(pl.multiple_of(place * SLOT, SLOT), SLOT)
        window[0, at, lanes] = low[0:SLOT]
        window[1, at, lanes] = low[BAND - SLOT:BAND]

    def message(rnd, way, half):
        lane = pl.ds(half * width, width)
        to = (other, neighbour(way))
        return (
            pltpu.make_async_remote_copy(send_f.at[rnd, way, 0, :, lane], recv_f.at[rnd, 1 - way, 0, :, lane], zsend.at[rnd, way, half],
                                         zrecv.at[rnd, 1 - way, half], device_id=to, device_id_type=MESH),
            pltpu.make_async_remote_copy(send_f.at[rnd, way, 1, :, lane], recv_f.at[rnd, 1 - way, 1, :, lane], fsend.at[rnd, way, half],
                                         frecv.at[rnd, 1 - way, half], device_id=to, device_id_type=MESH),
            pltpu.make_async_remote_copy(send_b.at[rnd, way, :, lane], recv_b.at[rnd, 1 - way, :, lane], bsend.at[rnd, way, half],
                                         brecv.at[rnd, 1 - way, half], device_id=to, device_id_type=MESH),
        )

    def update_edges(omega, half, rnd=None):
        for way in slow_first:
            x, y, third = (SUB - 1) * way, 1 + (SUB - 3) * way, 2 + (SUB - 5) * way
            link, next_link = 1 + (SUB - 2) * way, 2 + (SUB - 4) * way
            for lanes in lanes_of(half):
                first = res[x, :, lanes] - omega * neighbourless(x, lanes, ((y, link),))
                second = res[y, :, lanes] - omega * neighbourless(y, lanes, ((x, link), (third, next_link)))
                res[x, :, lanes] = first
                res[y, :, lanes] = second
                if rnd is not None:
                    send_f[rnd, way, 1, :, lanes] = first
                    send_b[rnd, way, :, lanes] = second.astype(BF16)
            if rnd is not None:
                @pl.when(present(way))
                def _():
                    for copy in message(rnd, way, half)[1:]:
                        copy.start()

    def update_inner(omega):
        def body(x, carry):
            for lanes in all_lanes:
                new = res[x, :, lanes] - omega * neighbourless(x, lanes, ((x - 1, x), (x + 1, x + 1)))
                res[x, :, lanes] = new
                put(w_in, x - 2, lanes, new)
            return carry
        lax.fori_loop(2, SUB - 2, body, 0)
        for way in range(2):
            for lanes in all_lanes:
                put(w_out, PLACES[way][3], lanes, res[SECOND_ROW[way], :, lanes])

    def presolve():
        for block in range(2):
            for part in range(0, CELLS, CHUNK):
                pre[block, part:part + CHUNK] = jnp.dot(s_in[block, part:part + CHUNK], w_in[block], preferred_element_type=F32)

    def take_edges(rnd, half, omega):
        for way in (1 - slow, slow):
            @pl.when(present(way))
            def _():
                if rnd == 0:
                    for block in range(2):
                        lane = pl.ds(half * width, width)
                        pltpu.make_async_remote_copy(send_0.at[way, block, :, lane], recv_0.at[way, block, :, lane], send0_sem.at[way, block, half],
                                                     recv0_sem.at[way, block, half], device_id=(other, neighbour(way)), device_id_type=MESH).wait_recv()
                        pltpu.make_async_remote_copy(low_0.at[way, block, :, lane], take_0.at[way, block, :, lane], low0_sem.at[way, block, half],
                                                     take0_sem.at[way, block, half], device_id=(other, neighbour(way)), device_id_type=MESH).wait_recv()
                else:
                    for copy in message(rnd - 1, 1 - way, half):
                        copy.wait_recv()
            x = (SUB - 1) * way
            face = face_x[SUB * way]
            for lanes in lanes_of(half):
                if rnd == 0:
                    z_far, r_far = [jnp.concatenate([recv_0[way, block, SUB * i:SUB * (i + 1), lanes] for block in range(2)], axis=0) for i in range(2)]
                    side = cross[way, 0] * (z_far - pltpu.roll(z_far, 1, 0))
                    r_far = r_far - side + pltpu.roll(side, BAND - 1, 0)
                    z_ends, r_ends = [[recv_0[way, block, 2 * SUB + i:2 * SUB + i + 1, lanes] for block in range(2)] for i in range(2)]
                    side = cross[way, 1, SUB:SUB + 1, :] * (z_ends[1] - z_ends[0])
                    r_beyond = jnp.concatenate([take_0[way, block, :, lanes].astype(F32) for block in range(2)], axis=0)
                    r_beyond = jnp.where(cell == SUB - 1, r_ends[0] + side, jnp.where(cell == SUB, r_ends[1] - side, r_beyond))
                else:
                    z_far = recv_f[rnd - 1, way, 0, :, lanes]
                    r_far = recv_f[rnd - 1, way, 1, :, lanes]
                    r_beyond = recv_b[rnd - 1, way, :, lanes]
                flux = omega * face * (cor[x, :, lanes] - z_far)
                new = res[x, :, lanes] - flux
                res[x, :, lanes] = new
                put(w_out, 7 * way, lanes, r_beyond)
                put(w_out, 1 + 5 * way, lanes, r_far + flux)
                put(w_out, 2 + 3 * way, lanes, new)

    def solve(block, part, lanes):
        return pre[block, part:part + CHUNK, lanes] + jnp.dot(s_out[block, part:part + CHUNK], w_out[block, :, lanes], preferred_element_type=F32)

    def rows_of(part):
        return ROW_ORDER[part // SUB:(part + CHUNK) // SUB]

    for load in (load_f, load_u):
        load.wait()
    for item in swaps[1:3]:
        item.wait()
    for half in range(HALVES):
        update_edges(1.0, half)
    update_inner(1.0)
    for block in range(2):
        for x in range(SUB):
            app[block, x] = cor[x, SUB * block:SUB * (block + 1), :]
    for item in swaps[3:]:
        item.wait()
    presolve()

    for way in range(2):
        @pl.when(has[way])
        def _():
            for block in range(2):
                pltpu.make_async_remote_copy(c_own.at[block, 0:8], c_nbr.at[way, block], csend.at[way, block], crecv.at[way, block],
                                             device_id=(other, near[way]), device_id_type=MESH).wait_recv()
        own = c_wide[EDGE_ROW[way]]
        beyond = [jnp.concatenate([column(c_nbr, (way, block), x) for block in range(2)], axis=0) for x in ((7, 6) if way == 0 else (0, 1))]
        face_x[0 if way == 0 else SUB] = 0.5 * (own + jnp.where(has[way], beyond[0], own))
        for i in range(2):
            cross[way, i] = jnp.where(cell == SUB, 0.5 * (beyond[i] + pltpu.roll(beyond[i], 1, 0)), 0.0)

    omega = om_ref[sys]
    for sweep in range(SWEEPS - 1):
        before = 1.0 if sweep == 0 else omega
        for half in range(HALVES):
            lanes = slice(half * width, (half + 1) * width)
            take_edges(sweep, half, before)
            for block in range(2):
                part = solve(block, 0, lanes)
                for i, x in enumerate(EDGE_ROWS):
                    cor[x, SUB * block:SUB * (block + 1), lanes] = part[SUB * i:SUB * (i + 1)]
                    if x in EDGE_ROW:
                        send_f[sweep, EDGE_ROW.index(x), 0, SUB * block:SUB * (block + 1), lanes] = part[SUB * i:SUB * (i + 1)]
            for way in slow_first:
                @pl.when(present(way))
                def _():
                    message(sweep, way, half)[0].start()
            update_edges(omega, half, sweep)
        for block in range(2):
            for x in EDGE_ROWS:
                app[block, x] = app[block, x] + omega * cor[x, SUB * block:SUB * (block + 1), :]
            for at in range(EDGE_CELLS, CELLS, CHUNK):
                part = solve(block, at, slice(0, RHS))
                for i, x in enumerate(rows_of(at)):
                    piece = part[SUB * i:SUB * (i + 1)]
                    cor[x, SUB * block:SUB * (block + 1), :] = piece
                    app[block, x] = app[block, x] + omega * piece
        update_inner(omega)
        presolve()

    for at in range(0, CELLS, CHUNK):
        for i, x in enumerate(rows_of(at)):
            here = slice(at + SUB * i, at + SUB * (i + 1))
            fin[x] = app[other, x] + omega * pre[other, here]
    early = pltpu.make_async_remote_copy(fin, fin_recv, back_send.at[HALVES], back_recv.at[HALVES], device_id={"col": other}, device_id_type=MESH)
    early.start()

    def back(half):
        lane = pl.ds(half * width, width)
        return pltpu.make_async_remote_copy(w_out.at[other, :, lane], w_fin.at[:, lane], back_send.at[half], back_recv.at[half],
                                            device_id={"col": other}, device_id_type=MESH)

    def finish_own(half):
        lanes = slice(half * width, (half + 1) * width)
        for at in range(0, CELLS, CHUNK):
            part = solve(core, at, lanes)
            for i, x in enumerate(rows_of(at)):
                out_ref[sys, x, :, lanes] = app[core, x, :, lanes] + omega * part[SUB * i:SUB * (i + 1)]

    def finish_other(half):
        lanes = slice(half * width, (half + 1) * width)
        back(half).wait()
        for at in range(0, CELLS, CHUNK):
            part = jnp.dot(so_swap[at:at + CHUNK], w_fin[:, lanes], preferred_element_type=F32)
            for i, x in enumerate(rows_of(at)):
                out_ref[1 - sys, x, :, lanes] = fin_recv[x, :, lanes] + their_omega * part[SUB * i:SUB * (i + 1)]

    their_omega = om_ref[1 - sys]
    take_edges(SWEEPS - 1, 0, omega)
    back(0).start()
    take_edges(SWEEPS - 1, 1, omega)
    back(1).start()
    finish_own(0)
    finish_own(1)
    early.wait()
    finish_other(0)
    finish_other(1)
    for way in range(2):
        @pl.when(has[way])
        def _():
            for j in range(2):
                coef_message(way, j).wait_send()
            for half in range(HALVES):
                for j in range(2):
                    for copy in start_message(way, j, half):
                        copy.wait_send()
                for rnd in range(SWEEPS - 1):
                    for copy in message(rnd, way, half):
                        copy.wait_send()


def solution(mesh):
    rows = mesh.shape["row"]
    grid_spec = P(None, "row", "col", None)

    def local_sweeps(forcing, init_guess, cell_coef, solve_rows, relax_factor):
        solve_mat = jnp.swapaxes(solve_rows.reshape(2, CELLS, EXT * EXT), 1, 2)
        any_space = pl.BlockSpec(memory_space=pl.ANY)
        rounds = SWEEPS - 1
        wide = (SUB, BAND, LANES)
        dma = pltpu.SemaphoreType.DMA
        held = [pltpu.with_memory_space_constraint(v, pltpu.HBM) for v in (forcing, init_guess, cell_coef, solve_mat, relax_factor)]
        return pl.pallas_call(
            functools.partial(kernel, rows),
            out_shape=jax.ShapeDtypeStruct(forcing.shape, F32),
            in_specs=[any_space] * 4 + [pl.BlockSpec(memory_space=pltpu.SMEM)],
            out_specs=pl.BlockSpec(memory_space=pltpu.VMEM),
            scratch_shapes=[
                pltpu.VMEM((SUB, BAND, RHS), F32),
                pltpu.VMEM((SUB, BAND, RHS), F32),
                pltpu.VMEM((2, SUB, SUB, RHS), F32),
                pltpu.VMEM((SUB, SUB, RHS), F32),
                pltpu.VMEM((2, CELLS, RHS), F32),
                pltpu.VMEM((2, EXT * EXT, CELLS), BF16),
                pltpu.VMEM((2, CELLS, OUTER * SLOT), BF16),
                pltpu.VMEM((2, CELLS, INNER * SLOT), BF16),
                pltpu.VMEM((2, OUTER * SLOT, RHS), BF16),
                pltpu.VMEM((2, INNER * SLOT, RHS), BF16),
                pltpu.VMEM((2, SUB, SUB), F32),
                pltpu.VMEM((2, SUB, SUB), F32),
                pltpu.VMEM((2, 2, 8, SUB), F32),
                pltpu.VMEM(wide, F32),
                pltpu.VMEM((2, SUB, SUB, LANES), F32),
                pltpu.VMEM((SUB + 1, BAND, LANES), F32),
                pltpu.VMEM(wide, F32),
                pltpu.VMEM(wide, F32),
                pltpu.VMEM((2, 2, BAND, LANES), F32),
                pltpu.VMEM(wide, F32),
                pltpu.VMEM((2, 2, 3, SUB, RHS), F32),
                pltpu.VMEM((2, 2, 2, SUB, RHS), F32),
                pltpu.VMEM((SUB, SUB, RHS), F32),
                pltpu.VMEM((SUB, SUB, RHS), F32),
                pltpu.VMEM((CELLS, OUTER * SLOT), BF16),
                pltpu.VMEM((CELLS, INNER * SLOT), BF16),
                pltpu.VMEM((OUTER * SLOT, RHS), BF16),
                pltpu.VMEM((SUB, SUB, RHS), F32),
                pltpu.VMEM((2, 2, FIRST, RHS), F32),
                pltpu.VMEM((2, 2, FIRST, RHS), F32),
                pltpu.VMEM((2, 2, SUB, RHS), BF16),
                pltpu.VMEM((2, 2, SUB, RHS), BF16),
                pltpu.VMEM((rounds, 2, 2, BAND, RHS), F32),
                pltpu.VMEM((rounds, 2, BAND, RHS), BF16),
                pltpu.VMEM((rounds, 2, 2, BAND, RHS), F32),
                pltpu.VMEM((rounds, 2, BAND, RHS), BF16),
                dma((6,)), dma((2,)), dma((2, 2, 2)), dma((5,)), dma((5,)), dma((2, 2)), dma((2, 2)), *[dma((2, 2, HALVES))] * 4,
                *[dma((rounds, 2, HALVES))] * 6,
                dma((HALVES + 1,)), dma((HALVES + 1,)),
            ],
            compiler_params=pltpu.CompilerParams(collective_id=0, has_side_effects=True, vmem_limit_bytes=40 * 1024 * 1024),
        )(*held)

    return jax.shard_map(local_sweeps, mesh=mesh, in_specs=(grid_spec, grid_spec, P(None, "row", "col"), P(None, "row", "col", None, None), P(None)), out_specs=grid_spec, check_vma=False)
```

```python
import functools

import jax
import jax.numpy as jnp
from jax import lax
from jax.experimental import pallas as pl
from jax.experimental.pallas import tpu as pltpu
from jax.sharding import PartitionSpec as P

SWEEPS = 4
SUB = 24
MARGIN = 2
EXT = SUB + 2 * MARGIN
BAND = 2 * SUB
SLOT = 32
OUTER = 8
INNER = EXT - OUTER
LANES = 128
RHS = 2 * LANES
HALVES = 2
F32 = jnp.float32
BF16 = jnp.bfloat16
MESH = pl.DeviceIdType.MESH

EDGE_ROWS = (0, 1, 2, SUB - 3, SUB - 2, SUB - 1)
ROW_ORDER = EDGE_ROWS + tuple(range(3, SUB - 3))
EDGE_CELLS = SUB * len(EDGE_ROWS)
CELLS = SUB * SUB
CHUNK = EDGE_CELLS
EDGE_ROW = (0, SUB - 1)
SECOND_ROW = (1, SUB - 2)
PLACES = ((0, 1, 2, 3), (7, 6, 5, 4))
FIRST = 2 * SUB + 8


def kernel(rows, f_hbm, u_hbm, c_hbm, s_hbm, om_ref, out_ref, res, cor, app, fin, pre, s_raw, s_out, s_in, w_out, w_in, c_own, c_raw, c_nbr,
           c_wide, c_part, face_x, face_lo, face_hi, cross, diag, u_edge, f_edge, f_swap, u_swap, so_swap, si_swap, w_fin, fin_recv, send_0, recv_0, low_0, take_0, send_f, send_b, recv_f, recv_b,
           loc_sem, s_sem, edge_sem, side_send, side_recv, csend, crecv, send0_sem, recv0_sem, low0_sem, take0_sem, zsend, zrecv, fsend, frecv, bsend, brecv, back_send, back_recv):
    core = lax.axis_index("col")
    row = lax.axis_index("row")
    other = 1 - core
    sys = lax.rem(core + row, 2)
    systems = (sys, 1 - sys)
    has = (row > 0, row < rows - 1)
    near = (jnp.maximum(row - 1, 0), jnp.minimum(row + 1, rows - 1))
    slow = (lax.rem(row, 4) == 3).astype(jnp.int32)
    slow_first = (slow, 1 - slow)

    def present(way):
        there = row + 2 * way - 1
        return (there >= 0) & (there < rows)

    def neighbour(way):
        return jnp.clip(row + 2 * way - 1, 0, rows - 1)
    mine = pl.multiple_of(core * SUB, 8)
    width = RHS // HALVES

    def lanes_of(half):
        return [slice(half * width + LANES * i, half * width + LANES * (i + 1)) for i in range(width // LANES)]

    all_lanes = [slice(LANES * i, LANES * (i + 1)) for i in range(RHS // LANES)]

    load_c = pltpu.make_async_copy(c_hbm, c_own, loc_sem.at[0])
    load_c.start()
    edge_loads = []
    for j in range(2):
        for way in range(2):
            edge_loads.append(pltpu.make_async_copy(u_hbm.at[systems[j], (SUB - 3) * way:(SUB - 3) * way + 3], u_edge.at[j, way], edge_sem.at[j, way, 0]))
            edge_loads.append(pltpu.make_async_copy(f_hbm.at[systems[j], (SUB - 2) * way:(SUB - 2) * way + 2], f_edge.at[j, way], edge_sem.at[j, way, 1]))
    for load in edge_loads:
        load.start()
    load_c_raw = pltpu.make_async_copy(c_hbm.at[sys], c_raw.at[core], loc_sem.at[4])
    load_s = [pltpu.make_async_copy(s_hbm.at[systems[j]], s_raw.at[j], s_sem.at[j]) for j in range(2)]
    load_f = pltpu.make_async_copy(f_hbm.at[sys], res.at[:, pl.ds(mine, SUB), :], loc_sem.at[1])
    load_u = pltpu.make_async_copy(u_hbm.at[sys], cor.at[:, pl.ds(mine, SUB), :], loc_sem.at[2])
    load_f_swap = pltpu.make_async_copy(f_hbm.at[1 - sys], f_swap, loc_sem.at[3])
    load_u_swap = pltpu.make_async_copy(u_hbm.at[1 - sys], u_swap, loc_sem.at[5])
    for load in (load_c_raw, load_s[1], load_f_swap, load_u_swap, load_s[0], load_f, load_u):
        load.start()

    barrier = pltpu.get_barrier_semaphore()
    for way in range(2):
        @pl.when(has[way])
        def _():
            for col in range(2):
                pl.semaphore_signal(barrier, inc=1, device_id=(col, neighbour(way)), device_id_type=MESH)
    pl.semaphore_signal(barrier, inc=1, device_id={"col": other}, device_id_type=MESH)

    eye = lax.broadcasted_iota(jnp.int32, (SUB, SUB), 0) == lax.broadcasted_iota(jnp.int32, (SUB, SUB), 1)

    def column(ref, lead, x):
        line = jnp.broadcast_to(ref[lead + (pl.ds(x, 1), slice(None))], (SUB, SUB))
        return jnp.broadcast_to(jnp.sum(jnp.where(eye, line, 0.0), axis=1, keepdims=True), (SUB, LANES))

    load_c.wait()
    for j in range(2):
        for x in EDGE_ROWS:
            c_part[j, x] = column(c_own, (systems[j],), x)
    for load in edge_loads:
        load.wait()
    spot = lax.broadcasted_iota(jnp.int32, (SUB, LANES), 0)
    tile_row = lax.broadcasted_iota(jnp.int32, (8, LANES), 0)
    for j in range(2):
        for way in range(2):
            step = 1 if way == 0 else -1
            place = (0, 1, 2) if way == 0 else (2, 1, 0)
            into = (0, 1) if way == 0 else (1, 0)
            at = [EDGE_ROW[way] + step * i for i in range(3)]
            c = [c_part[j, x] for x in at]
            link = [0.5 * (c[0] + c[1]), 0.5 * (c[1] + c[2])]
            for i in range(2):
                lo = jnp.where(spot == 0, 0.0, 0.5 * (c[i] + pltpu.roll(c[i], 1, 0)))
                hi = jnp.where(spot == SUB - 1, 0.0, 0.5 * (c[i] + pltpu.roll(c[i], SUB - 1, 0)))
                wall = jnp.where((spot == 0) & (core == 0) | (spot == SUB - 1) & (core == 1), c[i], 0.0)
                total = lo + hi + wall + link[i]
                if i == 1:
                    total = total + link[0]
                for lanes in all_lanes:
                    u = [u_edge[j, way, place[n], :, lanes] for n in range(3)]
                    flux = total * u[i] - lo * pltpu.roll(u[i], 1, 0) - hi * pltpu.roll(u[i], SUB - 1, 0) - link[i] * u[i + 1]
                    if i == 1:
                        flux = flux - link[0] * u[0]
                    part = f_edge[j, way, into[i], :, lanes] - flux
                    if i == 0:
                        send_0[way, j, 0:SUB, lanes] = u[0]
                        send_0[way, j, SUB:2 * SUB, lanes] = part
                    else:
                        low_0[way, j, :, lanes] = part.astype(BF16)
                        ends = [jnp.where(core == 0, v[SUB - 1:SUB], v[0:1]) for v in (u[1], part)]
                        send_0[way, j, 2 * SUB:FIRST, lanes] = jnp.where(tile_row == 0, ends[0], ends[1])

    source = lax.broadcasted_iota(jnp.int32, (4 * EXT, 4 * SLOT), 0)
    target = lax.broadcasted_iota(jnp.int32, (4 * EXT, 4 * SLOT), 1)
    ext_x = lax.shift_right_logical(source * 2341, 16)
    ext_y = source - EXT * ext_x

    shift = (SUB - (BAND - SLOT)) * core - MARGIN
    inside = ext_y + SUB * core - MARGIN
    hit = (target == ext_x * SLOT + ext_y + shift) & (inside >= 0) & (inside < BAND)
    pick = jnp.where(hit, 1.0, 0.0).astype(BF16)

    def reorder(j, outer, inner):
        groups = EXT // 4
        for group in range(groups):
            moved = lax.dot_general(s_raw[j, 4 * EXT * group:4 * EXT * (group + 1), :], pick, (((0,), (0,)), ((), ())), preferred_element_type=F32)
            cut = 3 * SUB
            moved = jnp.concatenate([moved[:cut], moved[-cut:], moved[cut:-cut]], axis=0).astype(BF16)
            if group == 0:
                outer[:, 0:4 * SLOT] = moved
            elif group == groups - 1:
                outer[:, 4 * SLOT:] = moved
            else:
                inner[:, 4 * SLOT * (group - 1):4 * SLOT * group] = moved

    load_s[1].wait()
    reorder(1, so_swap, si_swap)
    load_s[0].wait()
    reorder(0, s_out.at[core], s_in.at[core])
    load_f_swap.wait()
    load_u_swap.wait()

    pl.semaphore_wait(barrier, 1 + 2 * has[0].astype(jnp.int32) + 2 * has[1].astype(jnp.int32))

    def start_message(way, col, half):
        lane = pl.ds(half * width, width)
        j = other if col == 0 else core
        to = (col, neighbour(way))
        return (
            pltpu.make_async_remote_copy(send_0.at[way, j, :, lane], recv_0.at[1 - way, core, :, lane], send0_sem.at[way, col, half],
                                         recv0_sem.at[1 - way, core, half], device_id=to, device_id_type=MESH),
            pltpu.make_async_remote_copy(low_0.at[way, j, :, lane], take_0.at[1 - way, core, :, lane], low0_sem.at[way, col, half],
                                         take0_sem.at[1 - way, core, half], device_id=to, device_id_type=MESH),
        )

    def coef_message(way, col):
        there = lax.rem(sys + (other if col == 0 else core), 2)
        tile = pl.ds((SUB - 8) * way, 8)
        return pltpu.make_async_remote_copy(c_own.at[there, tile], c_nbr.at[1 - way, core], csend.at[way, col], crecv.at[1 - way, core],
                                            device_id=(col, neighbour(way)), device_id_type=MESH)

    for col in (1, 0):
        for half in range(HALVES):
            for way in slow_first:
                @pl.when(present(way))
                def _():
                    if half == 0:
                        coef_message(way, col).start()
                    for copy in start_message(way, col, half):
                        copy.start()

    def swap(src, dst, index):
        return pltpu.make_async_remote_copy(src, dst, side_send.at[index], side_recv.at[index], device_id={"col": other}, device_id_type=MESH)

    swaps = [
        swap(c_own.at[1 - sys], c_raw.at[core], 0),
        swap(u_swap, cor.at[:, pl.ds(mine, SUB), :], 1),
        swap(f_swap, res.at[:, pl.ds(mine, SUB), :], 2),
        swap(si_swap, s_in.at[core], 3),
        swap(so_swap, s_out.at[core], 4),
    ]
    for item in swaps:
        item.start()

    for way in range(2):
        @pl.when(jnp.logical_not(has[way]))
        def _():
            recv_0[way] = jnp.zeros(recv_0.shape[1:], F32)
            take_0[way] = jnp.zeros(take_0.shape[1:], BF16)
            c_nbr[way] = jnp.zeros(c_nbr.shape[1:], F32)
            for rnd in range(SWEEPS - 1):
                recv_f[rnd, way] = jnp.zeros(recv_f.shape[2:], F32)
                recv_b[rnd, way] = jnp.zeros(recv_b.shape[2:], BF16)

    load_c_raw.wait()
    swaps[0].wait()
    for x in range(SUB):
        for block in range(2):
            c_wide[x, SUB * block:SUB * (block + 1), :] = column(c_raw, (block,), x)
    cell = lax.broadcasted_iota(jnp.int32, (BAND, LANES), 0)
    for x in range(SUB):
        own = c_wide[x]
        lo = 0.5 * (own + pltpu.roll(own, 1, 0))
        hi = 0.5 * (own + pltpu.roll(own, BAND - 1, 0))
        total = jnp.where(cell == 0, own, lo) + jnp.where(cell == BAND - 1, own, hi)
        face_lo[x] = jnp.where(cell == 0, 0.0, lo)
        face_hi[x] = jnp.where(cell == BAND - 1, 0.0, hi)
        if x > 0:
            low_x = 0.5 * (c_wide[x - 1] + own)
            face_x[x] = low_x
            total = total + low_x
        if x < SUB - 1:
            total = total + 0.5 * (own + c_wide[x + 1])
        diag[x] = total

    def neighbourless(x, lanes, links):
        here = cor[x, :, lanes]
        flux = diag[x] * here - face_lo[x] * pltpu.roll(here, 1, 0) - face_hi[x] * pltpu.roll(here, BAND - 1, 0)
        for to, face in links:
            flux = flux - face_x[face] * cor[to, :, lanes]
        return flux

    def put(window, place, lanes, values):
        low = values.astype(BF16)
        at = pl.ds(place * SLOT, SLOT) if isinstance(place, int) else pl.ds(pl.multiple_of(place * SLOT, SLOT), SLOT)
        window[0, at, lanes] = low[0:SLOT]
        window[1, at, lanes] = low[BAND - SLOT:BAND]

    def message(rnd, way, half):
        lane = pl.ds(half * width, width)
        to = (other, neighbour(way))
        return (
            pltpu.make_async_remote_copy(send_f.at[rnd, way, 0, :, lane], recv_f.at[rnd, 1 - way, 0, :, lane], zsend.at[rnd, way, half],
                                         zrecv.at[rnd, 1 - way, half], device_id=to, device_id_type=MESH),
            pltpu.make_async_remote_copy(send_f.at[rnd, way, 1, :, lane], recv_f.at[rnd, 1 - way, 1, :, lane], fsend.at[rnd, way, half],
                                         frecv.at[rnd, 1 - way, half], device_id=to, device_id_type=MESH),
            pltpu.make_async_remote_copy(send_b.at[rnd, way, :, lane], recv_b.at[rnd, 1 - way, :, lane], bsend.at[rnd, way, half],
                                         brecv.at[rnd, 1 - way, half], device_id=to, device_id_type=MESH),
        )

    def update_edges(omega, half, rnd=None):
        for way in slow_first:
            x, y, third = (SUB - 1) * way, 1 + (SUB - 3) * way, 2 + (SUB - 5) * way
            link, next_link = 1 + (SUB - 2) * way, 2 + (SUB - 4) * way
            for lanes in lanes_of(half):
                first = res[x, :, lanes] - omega * neighbourless(x, lanes, ((y, link),))
                second = res[y, :, lanes] - omega * neighbourless(y, lanes, ((x, link), (third, next_link)))
                res[x, :, lanes] = first
                res[y, :, lanes] = second
                if rnd is not None:
                    send_f[rnd, way, 1, :, lanes] = first
                    send_b[rnd, way, :, lanes] = second.astype(BF16)
            if rnd is not None:
                @pl.when(present(way))
                def _():
                    for copy in message(rnd, way, half)[1:]:
                        copy.start()

    def update_inner(omega):
        def body(x, carry):
            for lanes in all_lanes:
                new = res[x, :, lanes] - omega * neighbourless(x, lanes, ((x - 1, x), (x + 1, x + 1)))
                res[x, :, lanes] = new
                put(w_in, x - 2, lanes, new)
            return carry
        lax.fori_loop(2, SUB - 2, body, 0)
        for way in range(2):
            for lanes in all_lanes:
                put(w_out, PLACES[way][3], lanes, res[SECOND_ROW[way], :, lanes])

    def presolve():
        for block in range(2):
            for part in range(0, CELLS, CHUNK):
                pre[block, part:part + CHUNK] = jnp.dot(s_in[block, part:part + CHUNK], w_in[block], preferred_element_type=F32)

    def take_edges(rnd, half, omega):
        for way in (1 - slow, slow):
            @pl.when(present(way))
            def _():
                if rnd == 0:
                    for block in range(2):
                        lane = pl.ds(half * width, width)
                        pltpu.make_async_remote_copy(send_0.at[way, block, :, lane], recv_0.at[way, block, :, lane], send0_sem.at[way, block, half],
                                                     recv0_sem.at[way, block, half], device_id=(other, neighbour(way)), device_id_type=MESH).wait_recv()
                        pltpu.make_async_remote_copy(low_0.at[way, block, :, lane], take_0.at[way, block, :, lane], low0_sem.at[way, block, half],
                                                     take0_sem.at[way, block, half], device_id=(other, neighbour(way)), device_id_type=MESH).wait_recv()
                else:
                    for copy in message(rnd - 1, 1 - way, half):
                        copy.wait_recv()
            x = (SUB - 1) * way
            face = face_x[SUB * way]
            for lanes in lanes_of(half):
                if rnd == 0:
                    z_far, r_far = [jnp.concatenate([recv_0[way, block, SUB * i:SUB * (i + 1), lanes] for block in range(2)], axis=0) for i in range(2)]
                    side = cross[way, 0] * (z_far - pltpu.roll(z_far, 1, 0))
                    r_far = r_far - side + pltpu.roll(side, BAND - 1, 0)
                    z_ends, r_ends = [[recv_0[way, block, 2 * SUB + i:2 * SUB + i + 1, lanes] for block in range(2)] for i in range(2)]
                    side = cross[way, 1, SUB:SUB + 1, :] * (z_ends[1] - z_ends[0])
                    r_beyond = jnp.concatenate([take_0[way, block, :, lanes].astype(F32) for block in range(2)], axis=0)
                    r_beyond = jnp.where(cell == SUB - 1, r_ends[0] + side, jnp.where(cell == SUB, r_ends[1] - side, r_beyond))
                else:
                    z_far = recv_f[rnd - 1, way, 0, :, lanes]
                    r_far = recv_f[rnd - 1, way, 1, :, lanes]
                    r_beyond = recv_b[rnd - 1, way, :, lanes]
                flux = omega * face * (cor[x, :, lanes] - z_far)
                new = res[x, :, lanes] - flux
                res[x, :, lanes] = new
                put(w_out, 7 * way, lanes, r_beyond)
                put(w_out, 1 + 5 * way, lanes, r_far + flux)
                put(w_out, 2 + 3 * way, lanes, new)

    def solve(block, part, lanes):
        return pre[block, part:part + CHUNK, lanes] + jnp.dot(s_out[block, part:part + CHUNK], w_out[block, :, lanes], preferred_element_type=F32)

    def rows_of(part):
        return ROW_ORDER[part // SUB:(part + CHUNK) // SUB]

    for load in (load_f, load_u):
        load.wait()
    for item in swaps[1:3]:
        item.wait()
    for half in range(HALVES):
        update_edges(1.0, half)
    update_inner(1.0)
    for block in range(2):
        for x in range(SUB):
            app[block, x] = cor[x, SUB * block:SUB * (block + 1), :]
    for item in swaps[3:]:
        item.wait()
    presolve()

    for way in range(2):
        @pl.when(has[way])
        def _():
            for block in range(2):
                pltpu.make_async_remote_copy(c_own.at[block, 0:8], c_nbr.at[way, block], csend.at[way, block], crecv.at[way, block],
                                             device_id=(other, near[way]), device_id_type=MESH).wait_recv()
        own = c_wide[EDGE_ROW[way]]
        beyond = [jnp.concatenate([column(c_nbr, (way, block), x) for block in range(2)], axis=0) for x in ((7, 6) if way == 0 else (0, 1))]
        face_x[0 if way == 0 else SUB] = 0.5 * (own + jnp.where(has[way], beyond[0], own))
        for i in range(2):
            cross[way, i] = jnp.where(cell == SUB, 0.5 * (beyond[i] + pltpu.roll(beyond[i], 1, 0)), 0.0)

    omega = om_ref[sys]
    for sweep in range(SWEEPS - 1):
        before = 1.0 if sweep == 0 else omega
        for half in range(HALVES):
            lanes = slice(half * width, (half + 1) * width)
            take_edges(sweep, half, before)
            for block in range(2):
                part = solve(block, 0, lanes)
                for i, x in enumerate(EDGE_ROWS):
                    cor[x, SUB * block:SUB * (block + 1), lanes] = part[SUB * i:SUB * (i + 1)]
                    if x in EDGE_ROW:
                        send_f[sweep, EDGE_ROW.index(x), 0, SUB * block:SUB * (block + 1), lanes] = part[SUB * i:SUB * (i + 1)]
            for way in slow_first:
                @pl.when(present(way))
                def _():
                    message(sweep, way, half)[0].start()
            update_edges(omega, half, sweep)
        for block in range(2):
            for x in EDGE_ROWS:
                app[block, x] = app[block, x] + omega * cor[x, SUB * block:SUB * (block + 1), :]
            for at in range(EDGE_CELLS, CELLS, CHUNK):
                part = solve(block, at, slice(0, RHS))
                for i, x in enumerate(rows_of(at)):
                    piece = part[SUB * i:SUB * (i + 1)]
                    cor[x, SUB * block:SUB * (block + 1), :] = piece
                    app[block, x] = app[block, x] + omega * piece
        update_inner(omega)
        presolve()

    for at in range(0, CELLS, CHUNK):
        for i, x in enumerate(rows_of(at)):
            here = slice(at + SUB * i, at + SUB * (i + 1))
            fin[x] = app[other, x] + omega * pre[other, here]
    early = pltpu.make_async_remote_copy(fin, fin_recv, back_send.at[HALVES], back_recv.at[HALVES], device_id={"col": other}, device_id_type=MESH)
    early.start()

    def back(half):
        lane = pl.ds(half * width, width)
        return pltpu.make_async_remote_copy(w_out.at[other, :, lane], w_fin.at[:, lane], back_send.at[half], back_recv.at[half],
                                            device_id={"col": other}, device_id_type=MESH)

    def finish_own(half):
        lanes = slice(half * width, (half + 1) * width)
        for at in range(0, CELLS, CHUNK):
            part = solve(core, at, lanes)
            for i, x in enumerate(rows_of(at)):
                out_ref[sys, x, :, lanes] = app[core, x, :, lanes] + omega * part[SUB * i:SUB * (i + 1)]

    def finish_other(half):
        lanes = slice(half * width, (half + 1) * width)
        back(half).wait()
        for at in range(0, CELLS, CHUNK):
            part = jnp.dot(so_swap[at:at + CHUNK], w_fin[:, lanes], preferred_element_type=F32)
            for i, x in enumerate(rows_of(at)):
                out_ref[1 - sys, x, :, lanes] = fin_recv[x, :, lanes] + their_omega * part[SUB * i:SUB * (i + 1)]

    their_omega = om_ref[1 - sys]
    take_edges(SWEEPS - 1, 0, omega)
    back(0).start()
    take_edges(SWEEPS - 1, 1, omega)
    back(1).start()
    finish_own(0)
    finish_own(1)
    early.wait()
    finish_other(0)
    finish_other(1)
    for way in range(2):
        @pl.when(has[way])
        def _():
            for j in range(2):
                coef_message(way, j).wait_send()
            for half in range(HALVES):
                for j in range(2):
                    for copy in start_message(way, j, half):
                        copy.wait_send()
                for rnd in range(SWEEPS - 1):
                    for copy in message(rnd, way, half):
                        copy.wait_send()


def solution(mesh):
    rows = mesh.shape["row"]
    grid_spec = P(None, "row", "col", None)

    def local_sweeps(forcing, init_guess, cell_coef, solve_rows, relax_factor):
        solve_mat = jnp.swapaxes(solve_rows.reshape(2, CELLS, EXT * EXT), 1, 2)
        any_space = pl.BlockSpec(memory_space=pl.ANY)
        rounds = SWEEPS - 1
        wide = (SUB, BAND, LANES)
        dma = pltpu.SemaphoreType.DMA
        held = [pltpu.with_memory_space_constraint(v, pltpu.HBM) for v in (forcing, init_guess, cell_coef, solve_mat, relax_factor)]
        return pl.pallas_call(
            functools.partial(kernel, rows),
            out_shape=jax.ShapeDtypeStruct(forcing.shape, F32),
            in_specs=[any_space] * 4 + [pl.BlockSpec(memory_space=pltpu.SMEM)],
            out_specs=pl.BlockSpec(memory_space=pltpu.VMEM),
            scratch_shapes=[
                pltpu.VMEM((SUB, BAND, RHS), F32),
                pltpu.VMEM((SUB, BAND, RHS), F32),
                pltpu.VMEM((2, SUB, SUB, RHS), F32),
                pltpu.VMEM((SUB, SUB, RHS), F32),
                pltpu.VMEM((2, CELLS, RHS), F32),
                pltpu.VMEM((2, EXT * EXT, CELLS), BF16),
                pltpu.VMEM((2, CELLS, OUTER * SLOT), BF16),
                pltpu.VMEM((2, CELLS, INNER * SLOT), BF16),
                pltpu.VMEM((2, OUTER * SLOT, RHS), BF16),
                pltpu.VMEM((2, INNER * SLOT, RHS), BF16),
                pltpu.VMEM((2, SUB, SUB), F32),
                pltpu.VMEM((2, SUB, SUB), F32),
                pltpu.VMEM((2, 2, 8, SUB), F32),
                pltpu.VMEM(wide, F32),
                pltpu.VMEM((2, SUB, SUB, LANES), F32),
                pltpu.VMEM((SUB + 1, BAND, LANES), F32),
                pltpu.VMEM(wide, F32),
                pltpu.VMEM(wide, F32),
                pltpu.VMEM((2, 2, BAND, LANES), F32),
                pltpu.VMEM(wide, F32),
                pltpu.VMEM((2, 2, 3, SUB, RHS), F32),
                pltpu.VMEM((2, 2, 2, SUB, RHS), F32),
                pltpu.VMEM((SUB, SUB, RHS), F32),
                pltpu.VMEM((SUB, SUB, RHS), F32),
                pltpu.VMEM((CELLS, OUTER * SLOT), BF16),
                pltpu.VMEM((CELLS, INNER * SLOT), BF16),
                pltpu.VMEM((OUTER * SLOT, RHS), BF16),
                pltpu.VMEM((SUB, SUB, RHS), F32),
                pltpu.VMEM((2, 2, FIRST, RHS), F32),
                pltpu.VMEM((2, 2, FIRST, RHS), F32),
                pltpu.VMEM((2, 2, SUB, RHS), BF16),
                pltpu.VMEM((2, 2, SUB, RHS), BF16),
                pltpu.VMEM((rounds, 2, 2, BAND, RHS), F32),
                pltpu.VMEM((rounds, 2, BAND, RHS), BF16),
                pltpu.VMEM((rounds, 2, 2, BAND, RHS), F32),
                pltpu.VMEM((rounds, 2, BAND, RHS), BF16),
                dma((6,)), dma((2,)), dma((2, 2, 2)), dma((5,)), dma((5,)), dma((2, 2)), dma((2, 2)), *[dma((2, 2, HALVES))] * 4,
                *[dma((rounds, 2, HALVES))] * 6,
                dma((HALVES + 1,)), dma((HALVES + 1,)),
            ],
            compiler_params=pltpu.CompilerParams(collective_id=0, has_side_effects=True, vmem_limit_bytes=40 * 1024 * 1024),
        )(*held)

    return jax.shard_map(local_sweeps, mesh=mesh, in_specs=(grid_spec, grid_spec, P(None, "row", "col"), P(None, "row", "col", None, None), P(None)), out_specs=grid_spec, check_vma=False)
```
